128 devices in a mesh: tenant: 32 (over z, x, y_lo), tp: 4 (over y_hi, core).
Axes of the slice: x: 4, y: 4 (y_hi: 2, y_lo: 2; y = y_hi * 2 + y_lo), z: 4, core: 2. Of those that a mesh axis runs over, the one named last changes fastest.
Arguments:
- src_tokens: bfloat16 [1536, 64, 1024], P('tenant'), may hold values from -64 to 64
- pair_tenant: int32 [1536], P('tenant'), may hold values from 0 to 31, as said below
- pair_length: int32 [1536], P('tenant'), may hold values from 1 to 64
- norm_gain: float32 [32, 1024], P('tenant'), may hold values from 0.1 to 1.9
- w_query: bfloat16 [32, 1024, 4096], P('tenant', None, 'tp'), may hold values from -1 to 1
- w_key: bfloat16 [32, 1024, 4096], P('tenant', None, 'tp'), may hold values from -1 to 1
- w_value: bfloat16 [32, 1024, 4096], P('tenant', None, 'tp'), may hold values from -0.1875 to 0.1875
- w_out: bfloat16 [32, 4096, 1024], P('tenant', 'tp'), may hold values from -0.09375 to 0.09375
- rel_bias: float32 [32, 32, 32], P('tenant', None, 'tp'), may hold values from -6 to 6
Outputs:
- layer_out: bfloat16 [65536, 1024], P(('tenant', 'tp'))
The draws below stay inside these ranges and needn't reach their ends.
Inputs may be any that keep to these rules, and one draw needn't show every extreme that they name: `pair_tenant`: the pairs of one retriever shard bound for one tenant have pair_length summing to at most 64; in every draw some tenant receives exactly 64 tokens from every shard.
All inputs are finite; a program needn't handle non-finite values.
Results may differ from the reference program's by a relative error of at most 0.0065.
Values may be sent and summed in bfloat16 or wider, within the bound.
A program may use at most 128 MiB of HBM per device.

```python
import math
import jax
import jax.numpy as jnp
import numpy as np
from jax import lax

D = 1024
HEADS = 32
DK = 128
BUCKETS = 32
CAP = 64
SHARD_PAIRS = 48
PAIRS_ALL = 1536
ROWS = 65536
N_TENANT = 32
N_TP = 4


def routing(key):
    mixed_key = jax.random.fold_in(key, 17)
    favored_key, tenant_key, length_key, pick_key = jax.random.split(mixed_key, 4)
    shard_count = PAIRS_ALL // SHARD_PAIRS
    favored = jax.random.randint(favored_key, (), 0, shard_count)
    picked = jax.random.randint(pick_key, (shard_count, 1), 0, SHARD_PAIRS)
    is_picked = jnp.arange(SHARD_PAIRS)[None, :] == picked
    tenant_grid = jax.random.randint(tenant_key, (shard_count, SHARD_PAIRS), 0, shard_count)
    tenant_grid = jnp.where(is_picked, favored, tenant_grid)
    same_tenant = tenant_grid[:, :, None] == tenant_grid[:, None, :]
    group_size = jnp.sum(same_tenant.astype(jnp.int32), axis=2)
    length_limit = CAP // group_size
    length_grid = jax.random.randint(length_key, (shard_count, SHARD_PAIRS), (length_limit + 1) // 2, length_limit + 1)
    in_group = (tenant_grid == favored) & jnp.logical_not(is_picked)
    others = jnp.sum(jnp.where(in_group, length_grid, 0), axis=1, keepdims=True)
    length_grid = jnp.where(is_picked, CAP - others, length_grid)
    return (tenant_grid.reshape(-1).astype(jnp.int32), length_grid.reshape(-1).astype(jnp.int32))


def draw_pair_tenant(key, part):
    return routing(key)[0]


def draw_pair_length(key, part):
    return routing(key)[1]


def query_key_pair(key):
    mixed_key = jax.random.fold_in(key, 29)
    first_key, second_key = jax.random.split(mixed_key, 2)
    tenant_count = PAIRS_ALL // SHARD_PAIRS
    array_shape = (tenant_count, D, HEADS * DK)
    fan_scale = 1.0 / math.sqrt(D)
    score_scale = 1.0 / math.sqrt(DK)
    first_draw = jax.random.normal(first_key, array_shape, jnp.float32) * fan_scale
    second_draw = jax.random.normal(second_key, array_shape, jnp.float32) * fan_scale
    return (jnp.clip(first_draw, -1.0, 1.0) * score_scale, jnp.clip(second_draw, -1.0, 1.0))


def draw_w_query(key, part):
    return query_key_pair(key)[0].astype(jnp.bfloat16)


def draw_w_key(key, part):
    return query_key_pair(key)[1].astype(jnp.bfloat16)


def draw_src_tokens(key, part):
    base_key = jax.random.fold_in(jax.random.fold_in(key, 41), 0)
    normal_values = jax.random.normal(base_key, (PAIRS_ALL, CAP, D), jnp.float32)
    return jnp.clip(normal_values, -6.0, 6.0).astype(jnp.bfloat16)


def block_levels(rng, shape, cuts, low, top_value):
    loudness, own = 1.0, jax.random.fold_in(rng, 6)
    for dim, shards_of in cuts:
        steps = jnp.exp(jax.random.uniform(jax.random.fold_in(own, dim), (shards_of,), jnp.float32, low / len(cuts), top_value / len(cuts)))
        loudness = loudness * jnp.repeat(steps, shape[dim] // shards_of).reshape([-1 if axis == dim else 1 for axis in range(len(shape))])
    return loudness


def bell_draw(rng, shape, width, most, cuts=(), kind=jnp.bfloat16):
    array = width * jax.random.normal(rng, shape, jnp.float32)
    if cuts:
        array = array * block_levels(rng, shape, cuts, -0.22, 0.18)
    return jnp.clip(array, -most, most).astype(kind)


def setup_inputs(seed: int = 0) -> dict:
    splits = jax.random.split(jax.random.key(seed), 10)
    return {
        "src_tokens": draw_src_tokens(jax.random.fold_in(splits[9], 71), 0),
        "pair_tenant": draw_pair_tenant(jax.random.fold_in(splits[9], 71), 0),
        "pair_length": draw_pair_length(jax.random.fold_in(splits[9], 71), 0),
        "norm_gain": jnp.clip(1.0 + 0.18 * jax.random.normal(splits[3], (N_TENANT, D), jnp.float32), 0.1, 1.9),
        "w_query": draw_w_query(jax.random.fold_in(splits[9], 71), 0),
        "w_key": draw_w_key(jax.random.fold_in(splits[9], 71), 0),
        "w_value": bell_draw(splits[6], (N_TENANT, D, HEADS * DK), D ** -0.5, 0.1875, ((0, 32), (2, 4))),
        "w_out": bell_draw(splits[7], (N_TENANT, HEADS * DK, D), (HEADS * DK) ** -0.5, 0.09375, ((0, 32), (1, 4))),
        "rel_bias": bell_draw(splits[8], (N_TENANT, BUCKETS, HEADS), 1.0, 6.0, ((0, 32), (2, 4)), jnp.float32),
    }


def bucket_grid(extent, buckets):
    offsets = np.arange(extent)[None, :] - np.arange(extent)[:, None]
    half_count = buckets // 2
    upward = np.where(offsets > 0, half_count, 0)
    distance = np.abs(offsets)
    exact_limit = half_count // 2
    ratio = np.maximum(distance, 1) / exact_limit
    spread_bucket = exact_limit + np.floor(np.log(ratio) / math.log(128.0 / exact_limit) * (half_count - exact_limit)).astype(np.int32)
    spread_bucket = np.minimum(spread_bucket, half_count - 1)
    return (upward + np.where(distance < exact_limit, distance, spread_bucket)).astype(np.int32)

def rms_normed(tenant_rows, gain_row):
    values = tenant_rows.astype(jnp.float32)
    mean_square = lax.optimization_barrier(jnp.mean(values * values, axis=-1, keepdims=True))
    return (values * lax.rsqrt(mean_square + 1e-06) * gain_row).astype(jnp.bfloat16)

def reference(src_tokens, pair_tenant, pair_length, norm_gain, w_query, w_key, w_value, w_out, rel_bias):
    shard_pairs = PAIRS_ALL // N_TENANT
    tenant_grid = pair_tenant.reshape(N_TENANT, shard_pairs).astype(jnp.int32)
    length_grid = pair_length.reshape(N_TENANT, shard_pairs).astype(jnp.int32)
    pair_order = jnp.arange(shard_pairs, dtype=jnp.int32)
    earlier = (tenant_grid[:, :, None] == tenant_grid[:, None, :]) & (pair_order[None, None, :] < pair_order[None, :, None])
    offset = lax.optimization_barrier(jnp.sum(jnp.where(earlier, length_grid[:, None, :], 0), axis=2)).astype(jnp.int32)
    source = jnp.arange(N_TENANT, dtype=jnp.int32)[:, None]
    start_row = ((tenant_grid * N_TENANT + source) * CAP + offset).astype(jnp.int32)
    position = jnp.arange(CAP, dtype=jnp.int32)
    target = start_row[:, :, None] + position[None, None, :]
    target = jnp.where(position[None, None, :] < length_grid[:, :, None], target, ROWS).reshape(-1).astype(jnp.int32)
    packed = jnp.zeros((ROWS, D), jnp.bfloat16).at[target].set(src_tokens.reshape(-1, D), mode='drop')
    pair_ids = jnp.broadcast_to(jnp.arange(PAIRS_ALL, dtype=jnp.int32)[:, None], (PAIRS_ALL, CAP)).reshape(-1)
    segment = jnp.full((ROWS,), -1, jnp.int32).at[target].set(pair_ids, mode='drop')
    bucket_index = jnp.asarray(bucket_grid(CAP, BUCKETS))
    group_width = HEADS * DK // N_TP
    tenant_count_rows = N_TENANT * CAP

    def one_tenant(inputs):
        tenant_rows, tenant_segment, gain_row, query_weight, key_weight, value_weight, out_weight, bias_table = inputs
        normed = rms_normed(tenant_rows, gain_row)
        query_rows = jnp.dot(normed, query_weight, preferred_element_type=jnp.float32).astype(jnp.bfloat16)
        key_rows = jnp.dot(normed, key_weight, preferred_element_type=jnp.float32).astype(jnp.bfloat16)
        value_rows = jnp.dot(normed, value_weight, preferred_element_type=jnp.float32).astype(jnp.bfloat16)
        query_blocks = query_rows.reshape(N_TENANT, CAP, HEADS, DK).astype(jnp.float32)
        key_blocks = key_rows.reshape(N_TENANT, CAP, HEADS, DK).astype(jnp.float32)
        value_blocks = value_rows.reshape(N_TENANT, CAP, HEADS, DK).astype(jnp.float32)
        position_bias = jnp.transpose(bias_table[bucket_index], (2, 0, 1))
        scores = jnp.einsum('bqhd,bkhd->bhqk', query_blocks, key_blocks, precision=lax.Precision.HIGHEST)
        scores = scores + position_bias[None]
        segment_blocks = tenant_segment.reshape(N_TENANT, CAP)
        allowed = (segment_blocks[:, :, None] == segment_blocks[:, None, :]) & (segment_blocks[:, None, :] >= 0)
        scores = jnp.where(allowed[:, None], scores, -1000000000.0)
        maxima = lax.optimization_barrier(jnp.max(scores, axis=-1, keepdims=True))
        weights = jnp.exp(scores - maxima)
        probabilities = (weights / lax.optimization_barrier(jnp.sum(weights, axis=-1, keepdims=True))).astype(jnp.bfloat16)
        context = jnp.einsum('bhqk,bkhd->bqhd', probabilities.astype(jnp.float32), value_blocks, precision=lax.Precision.HIGHEST)
        context = context.astype(jnp.bfloat16).reshape(tenant_count_rows, N_TP, group_width)
        partials = jnp.einsum('rgi,gid->grd', context.astype(jnp.float32), out_weight.reshape(N_TP, group_width, D).astype(jnp.float32), precision=lax.Precision.HIGHEST)
        partials = lax.optimization_barrier(partials.astype(jnp.bfloat16)).astype(jnp.float32)
        total = tenant_rows.astype(jnp.float32) + lax.optimization_barrier(jnp.sum(partials, axis=0))
        return jnp.where(tenant_segment[:, None] >= 0, total, 0.0).astype(jnp.bfloat16)
    outputs = lax.map(one_tenant, (packed.reshape(N_TENANT, tenant_count_rows, D), segment.reshape(N_TENANT, tenant_count_rows), norm_gain, w_query, w_key, w_value, w_out, rel_bias))
    return outputs.reshape(ROWS, D)
```

```python
import functools
import math

import jax
import jax.numpy as jnp
import numpy as np
from jax import lax
from jax.experimental import pallas as pl
from jax.experimental.pallas import tpu as pltpu
from jax.sharding import PartitionSpec as P

MESH = pl.DeviceIdType.MESH
CAP = 64
D = 1024
HALF = 512
SLOTS = 32
GROUPS = 8
HEADS = 8
DK = 128
NEG = -1e30
EPS = 1e-6


def bucket_grid(extent, buckets):
    offsets = np.arange(extent)[None, :] - np.arange(extent)[:, None]
    half_count = buckets // 2
    upward = np.where(offsets > 0, half_count, 0)
    distance = np.abs(offsets)
    exact_limit = half_count // 2
    ratio = np.maximum(distance, 1) / exact_limit
    spread_bucket = exact_limit + np.floor(
        np.log(ratio) / math.log(128.0 / exact_limit) * (half_count - exact_limit)
    ).astype(np.int32)
    spread_bucket = np.minimum(spread_bucket, half_count - 1)
    return (upward + np.where(distance < exact_limit, distance, spread_bucket)).astype(np.int32)


def position_bias(table):
    grid = bucket_grid(CAP, table.shape[0])
    grid = np.concatenate([grid, grid], axis=1)
    match = jnp.asarray(
        (grid[:, :, None] == np.arange(table.shape[0])[None, None, :]).astype(np.float32)
    )
    return jnp.einsum("qkb,bh->hqk", match, table, precision=lax.Precision.HIGHEST)


def pack_kernel(tenant_ref, length_ref, src_ref, packed_ref, meta_ref, tokens, stage, fill, sems):
    core = lax.rem(lax.axis_index("tp"), 2)
    pairs = src_ref.shape[0]
    step = pairs // 4
    copies = []
    for i in range(4):
        copies.append(
            pltpu.make_async_copy(
                src_ref.at[pl.ds(i * step, step), :, pl.ds(pl.multiple_of(core * HALF, HALF), HALF)],
                tokens.at[pl.ds(i * step, step)],
                sems.at[i],
            )
        )
        copies[-1].start()

    def clear(u, _):
        fill[u] = 0
        return 0

    lax.fori_loop(0, SLOTS, clear, 0)
    meta_ref[...] = jnp.zeros_like(meta_ref)
    lane = lax.broadcasted_iota(jnp.int32, (1, 128), 1)

    def place(i, _):
        u = tenant_ref[i]
        n = length_ref[i]
        start = fill[u]
        fill[u] = start + n
        code = start * 256 + start + n
        inside = ((lane % CAP) >= start) & ((lane % CAP) < start + n)
        meta_ref[u] = jnp.where(inside, code, meta_ref[u])
        for c in range(4):
            piece = tokens[i, :, c * 128 : c * 128 + 128].astype(jnp.float32)
            stage[u, c, pl.ds(start, CAP), :] = piece
        return 0

    for i in range(4):
        copies[i].wait()
        lax.fori_loop(i * step, (i + 1) * step, place, 0)
    row = lax.broadcasted_iota(jnp.int32, (CAP, 128), 0)

    def finish(u, _):
        for c in range(4):
            rows = jnp.where(row < fill[u], stage[u, c, 0:CAP, :], 0.0).astype(jnp.bfloat16)
            packed_ref[u, :, c * 128 : c * 128 + 128] = rows
        return 0

    lax.fori_loop(0, SLOTS, finish, 0)


def pack(tenant, length, tokens):
    pairs = tokens.shape[0]
    smem = pl.BlockSpec(memory_space=pltpu.SMEM)
    vmem = pl.BlockSpec(memory_space=pltpu.VMEM)
    return pl.pallas_call(
        pack_kernel,
        out_shape=(
            jax.ShapeDtypeStruct((SLOTS, CAP, HALF), jnp.bfloat16),
            jax.ShapeDtypeStruct((SLOTS, 1, 128), jnp.int32),
        ),
        in_specs=[smem, smem, pl.BlockSpec(memory_space=pl.ANY)],
        out_specs=(vmem, vmem),
        scratch_shapes=[
            pltpu.VMEM((pairs, CAP, HALF), jnp.bfloat16),
            pltpu.VMEM((SLOTS, 4, 2 * CAP, 128), jnp.float32),
            pltpu.SMEM((SLOTS,), jnp.int32),
            pltpu.SemaphoreType.DMA((4,)),
        ],
        compiler_params=pltpu.CompilerParams(vmem_limit_bytes=40 * 1024 * 1024),
        name="pack",
    )(tenant, length, tokens)


def here():
    t = lax.axis_index("tenant")
    p = lax.axis_index("tp")
    return t // 8, (t // 2) % 4, t % 2, p // 2, p % 2


def device(z, x, lo, hi, core):
    return ((z % 4) * 8 + (x % 4) * 2 + lo % 2, (hi % 2) * 2 + core % 2)


def shift_of(pos):
    g = pos // 4
    a = (pos // 2) % 2
    b = pos % 2
    dz = g % 2 + 2 * a
    dx = (g // 2 + b) % 4
    return dz, dx, b


def layer_kernel(
    packed_ref, meta_ref, gain_ref, bias_ref, wq_hbm, wk_hbm, wv_hbm, wo_hbm, out_ref,
    wq, wk, wv, wo, arr, codes, normed, query, key, value, context, part,
    keep, pair_out, pair_in, mate_out, mate_in, far_out, far_in, mine,
    wsem, tok_s, tok_r, meta_s, meta_r, fwd_s, fwd_r,
    pair_s, pair_r, mate_s, mate_r, far_s, far_r,
):
    z, x, lo, hi, core = here()
    tenant = lax.axis_index("tenant")
    partner = device(z, x, lo, hi, core + 1)

    def peer(pos):
        dz, dx, dl = shift_of(pos)
        return device(z + dz, x + dx, lo + dl, hi + dl * ((dz + dx) % 2), core)

    weights = [
        pltpu.make_async_copy(src.at[0], dst, wsem.at[i])
        for i, (src, dst) in enumerate(((wq_hbm, wq), (wk_hbm, wk), (wv_hbm, wv), (wo_hbm, wo)))
    ]
    for copy in weights:
        copy.start()

    barrier = pltpu.get_barrier_semaphore()

    def greet(pos, _):
        pl.semaphore_signal(barrier, inc=1, device_id=peer(pos), device_id_type=MESH)
        return 0

    lax.fori_loop(1, SLOTS, greet, 0)
    pl.semaphore_signal(barrier, inc=1, device_id=partner, device_id_type=MESH)
    for c in range(2):
        pl.semaphore_signal(
            barrier, inc=1, device_id=device(z, x, lo, hi + 1, c), device_id_type=MESH
        )
    pl.semaphore_wait(barrier, SLOTS + 2)

    def token_copy(pos):
        target = peer(pos)
        return pltpu.make_async_remote_copy(
            packed_ref.at[target[0]], arr.at[core, pos], tok_s.at[pos], tok_r.at[pos],
            device_id=target, device_id_type=MESH,
        )

    def meta_copy(pos):
        target = peer(pos)
        return pltpu.make_async_remote_copy(
            meta_ref.at[target[0]], codes.at[pos], meta_s.at[pos], meta_r.at[pos],
            device_id=target, device_id_type=MESH,
        )

    def forward_copy(pos):
        return pltpu.make_async_remote_copy(
            arr.at[core, pos], arr.at[core, pos], fwd_s.at[pos], fwd_r.at[pos],
            device_id=partner, device_id_type=MESH,
        )

    own_forward = pltpu.make_async_remote_copy(
        packed_ref.at[tenant], arr.at[core, 0], fwd_s.at[0], fwd_r.at[0],
        device_id=partner, device_id_type=MESH,
    )
    def wait_partner(pos):
        pltpu.make_async_remote_copy(
            arr.at[1 - core, pos], arr.at[1 - core, pos], fwd_s.at[pos], fwd_r.at[pos],
            device_id=partner, device_id_type=MESH,
        ).wait_recv()

    own_forward.start()

    def send(pos, _):
        meta_copy(pos).start()
        token_copy(pos).start()
        return 0

    lax.fori_loop(1, SLOTS, send, 0)
    arr[core, 0] = packed_ref[tenant]
    codes[0] = meta_ref[tenant]

    def receive(pos):
        token_copy(pos).wait_recv()
        meta_copy(pos).wait_recv()
        forward_copy(pos).start()

    for pos in range(1, 4):
        receive(pos)

    def planes(g):
        first = (z + 4 - g % 2) % 4
        other = (first + 2) % 4
        first_far = jnp.where(first // 2 != hi, 1, 0)
        far_pair = 1 - first_far
        far_plane = jnp.where(first_far == 1, first, other)
        near_plane = jnp.where(first_far == 1, other, first)
        return far_pair, far_plane, near_plane

    def pair_copy(g):
        return pltpu.make_async_remote_copy(
            pair_out.at[g], pair_in.at[g], pair_s.at[g], pair_r.at[g],
            device_id=partner, device_id_type=MESH,
        )

    def mate_copy(q):
        return pltpu.make_async_remote_copy(
            mate_out.at[q], mate_in.at[q], mate_s.at[q], mate_r.at[q],
            device_id=partner, device_id_type=MESH,
        )

    def far_copy(g):
        _, far_plane, _ = planes(g)
        return pltpu.make_async_remote_copy(
            far_out.at[g], far_in.at[core, g // 2], far_s.at[g], far_r.at[core, g // 2],
            device_id=device(z, x, lo, hi + 1, far_plane), device_id_type=MESH,
        )

    def finish_pair(g):
        pair_copy(g).wait_recv()
        total = keep[g % 2] + pair_in[g].astype(jnp.float32)
        far_out[g] = total.astype(jnp.bfloat16)
        far_copy(g).start()

    row = lax.broadcasted_iota(jnp.int32, (128, 128), 0)
    col = lax.broadcasted_iota(jnp.int32, (128, 128), 1)

    def group(g, _):
        base = g * 4
        for i in range(4):
            wait_partner(base + i)
        left = arr[0, pl.ds(base, 4)].reshape(256, HALF).astype(jnp.float32)
        right = arr[1, pl.ds(base, 4)].reshape(256, HALF).astype(jnp.float32)
        mean = (
            jnp.sum(left * left, axis=-1, keepdims=True)
            + jnp.sum(right * right, axis=-1, keepdims=True)
        ) / D
        scale = lax.rsqrt(mean + EPS)
        normed[:, 0:HALF] = (left * scale * gain_ref[:, 0:HALF]).astype(jnp.bfloat16)
        normed[:, HALF:D] = (right * scale * gain_ref[:, HALF:D]).astype(jnp.bfloat16)

        @pl.when(g == 0)
        def _():
            for copy in weights:
                copy.wait()

        rows = normed[...]
        query[...] = jnp.dot(rows, wq[...], preferred_element_type=jnp.float32).astype(jnp.bfloat16)
        key[...] = jnp.dot(rows, wk[...], preferred_element_type=jnp.float32).astype(jnp.bfloat16)
        value[...] = jnp.dot(rows, wv[...], preferred_element_type=jnp.float32).astype(jnp.bfloat16)

        @pl.when(g > 0)
        def _():
            finish_pair(g - 1)

        @pl.when(g < GROUPS - 1)
        def _():
            for i in range(4):
                receive(base + 4 + i)

        for block in range(2):
            code = jnp.where(col[0:1] < CAP, codes[base + 2 * block], codes[base + 2 * block + 1])
            shift = jnp.where(col[0:1] < CAP, 0, CAP)
            start = code // 256 + shift
            end = code % 256 + shift
            allowed = (row >= start) & (row < end)
            span = slice(block * 128, block * 128 + 128)
            for h in range(HEADS):
                lanes = slice(h * DK, h * DK + DK)
                s = lax.dot_general(
                    query[span, lanes], key[span, lanes], (((1,), (1,)), ((), ())),
                    preferred_element_type=jnp.float32,
                )
                b = bias_ref[h]
                s = jnp.where(allowed, s + jnp.concatenate([b, b], axis=0), NEG)
                top = jnp.max(s, axis=-1, keepdims=True)
                w = jnp.exp(s - top)
                total = jnp.sum(w, axis=-1, keepdims=True)
                inverse = jnp.where(top > 0.5 * NEG, 1.0 / total, 0.0)
                ctx = jnp.dot(
                    (w * inverse).astype(jnp.bfloat16), value[span, lanes],
                    preferred_element_type=jnp.float32,
                )
                context[span, lanes] = ctx.astype(jnp.bfloat16)

        part[...] = jnp.dot(context[...], wo[...], preferred_element_type=jnp.float32)
        far_pair, _, near_plane = planes(g)
        far_rows = pl.ds(pl.multiple_of(far_pair * 128, 128), 128)
        near_rows = pl.ds(pl.multiple_of((1 - far_pair) * 128, 128), 128)
        own_cols = pl.ds(pl.multiple_of(core * HALF, HALF), HALF)
        other_cols = pl.ds(pl.multiple_of((1 - core) * HALF, HALF), HALF)
        pair_out[g] = part[far_rows, other_cols].astype(jnp.bfloat16)
        pair_copy(g).start()
        keep[g % 2] = part[far_rows, own_cols]

        @pl.when(near_plane % 2 == core)
        def _():
            mine[g // 2] = part[near_rows, :]

        @pl.when(near_plane % 2 != core)
        def _():
            mate_out[g // 2] = part[near_rows, :].astype(jnp.bfloat16)
            mate_copy(g // 2).start()

        return 0

    lax.fori_loop(0, GROUPS, group, 0)
    finish_pair(GROUPS - 1)

    plane = hi * 2 + core
    parity = (z + plane) % 2

    def combine(q, _):
        g = 2 * q + parity
        far_pair, _, _ = planes(g)
        near_pair = 1 - far_pair
        mate_copy(q).wait_recv()
        for c in range(2):
            pltpu.make_async_remote_copy(
                far_in.at[c, q], far_in.at[c, q], far_s.at[q], far_r.at[c, q],
                device_id=partner, device_id_type=MESH,
            ).wait_recv()
        for b in range(2):
            pos = g * 4 + near_pair * 2 + b
            src_slot = ((x + 8 - q - b) % 4) * 2 + (lo + b) % 2
            span = slice(b * CAP, b * CAP + CAP)
            for c in range(2):
                cols = slice(c * HALF, c * HALF + HALF)
                total = (
                    mine[q, span, cols]
                    + mate_in[q, span, cols].astype(jnp.float32)
                    + far_in[c, q, span, :].astype(jnp.float32)
                    + arr[c, pos].astype(jnp.float32)
                )
                out_ref[src_slot, :, cols] = total.astype(jnp.bfloat16)
        return 0

    lax.fori_loop(0, 4, combine, 0)

    def drain(pos, _):
        token_copy(pos).wait_send()
        meta_copy(pos).wait_send()
        forward_copy(pos).wait_send()
        return 0

    own_forward.wait_send()
    lax.fori_loop(1, SLOTS, drain, 0)

    def drain_groups(g, _):
        pair_copy(g).wait_send()
        far_copy(g).wait_send()
        return 0

    lax.fori_loop(0, GROUPS, drain_groups, 0)

    def drain_mates(q, _):
        mate_copy(q).wait_send()
        return 0

    lax.fori_loop(0, 4, drain_mates, 0)


def layer(packed, meta, gain, bias, wq, wk, wv, wo):
    vmem = pl.BlockSpec(memory_space=pltpu.VMEM)
    anywhere = pl.BlockSpec(memory_space=pl.ANY)
    bf, f32 = jnp.bfloat16, jnp.float32
    dma = pltpu.SemaphoreType.DMA
    return pl.pallas_call(
        layer_kernel,
        out_shape=jax.ShapeDtypeStruct((8, CAP, D), bf),
        in_specs=[vmem] * 4 + [anywhere] * 4,
        out_specs=vmem,
        scratch_shapes=[pltpu.VMEM((D, D), bf)] * 4
        + [
            pltpu.VMEM((2, SLOTS, CAP, HALF), bf),
            pltpu.VMEM((SLOTS, 1, 128), jnp.int32),
        ]
        + [pltpu.VMEM((256, D), bf)] * 5
        + [
            pltpu.VMEM((256, D), f32),
            pltpu.VMEM((2, 128, HALF), f32),
            pltpu.VMEM((GROUPS, 128, HALF), bf),
            pltpu.VMEM((GROUPS, 128, HALF), bf),
            pltpu.VMEM((4, 128, D), bf),
            pltpu.VMEM((4, 128, D), bf),
            pltpu.VMEM((GROUPS, 128, HALF), bf),
            pltpu.VMEM((2, 4, 128, HALF), bf),
            pltpu.VMEM((4, 128, D), f32),
            dma((4,)), dma((SLOTS,)), dma((SLOTS,)), dma((SLOTS,)), dma((SLOTS,)),
            dma((SLOTS,)), dma((SLOTS,)),
            dma((GROUPS,)), dma((GROUPS,)), dma((4,)), dma((4,)), dma((GROUPS,)), dma((2, 4)),
        ],
        compiler_params=pltpu.CompilerParams(
            collective_id=0, has_side_effects=True, vmem_limit_bytes=56 * 1024 * 1024
        ),
        name="layer",
    )(packed, meta, gain, bias, wq, wk, wv, wo)


def per_device(
    src_tokens, pair_tenant, pair_length, norm_gain, w_query, w_key, w_value, w_out, rel_bias
):
    packed, meta = pack(pair_tenant, pair_length, src_tokens)
    bias = position_bias(rel_bias[0])
    out = layer(packed, meta, norm_gain, bias, w_query, w_key, w_value, w_out)
    return out.reshape(8 * CAP, D)


def solution(mesh):
    in_specs = (
        P("tenant", None, None),
        P("tenant"),
        P("tenant"),
        P("tenant", None),
        P("tenant", None, "tp"),
        P("tenant", None, "tp"),
        P("tenant", None, "tp"),
        P("tenant", "tp", None),
        P("tenant", None, "tp"),
    )
    out_specs = P(("tenant", "tp"), None)
    return jax.shard_map(
        per_device, mesh=mesh, in_specs=in_specs, out_specs=out_specs, check_vma=False
    )
```

```python
import functools
import math

import jax
import jax.numpy as jnp
import numpy as np
from jax import lax
from jax.experimental import pallas as pl
from jax.experimental.pallas import tpu as pltpu
from jax.sharding import PartitionSpec as P

MESH = pl.DeviceIdType.MESH
CAP = 64
D = 1024
HALF = 512
SLOTS = 32
GROUPS = 8
HEADS = 8
DK = 128
NEG = -1e30
EPS = 1e-6


def bucket_grid(extent, buckets):
    offsets = np.arange(extent)[None, :] - np.arange(extent)[:, None]
    half_count = buckets // 2
    upward = np.where(offsets > 0, half_count, 0)
    distance = np.abs(offsets)
    exact_limit = half_count // 2
    ratio = np.maximum(distance, 1) / exact_limit
    spread_bucket = exact_limit + np.floor(
        np.log(ratio) / math.log(128.0 / exact_limit) * (half_count - exact_limit)
    ).astype(np.int32)
    spread_bucket = np.minimum(spread_bucket, half_count - 1)
    return (upward + np.where(distance < exact_limit, distance, spread_bucket)).astype(np.int32)


def position_bias(table):
    grid = bucket_grid(CAP, table.shape[0])
    grid = np.concatenate([grid, grid], axis=1)
    match = jnp.asarray(
        (grid[:, :, None] == np.arange(table.shape[0])[None, None, :]).astype(np.float32)
    )
    return jnp.einsum("qkb,bh->hqk", match, table, precision=lax.Precision.HIGHEST)


def pack_kernel(tenant_ref, length_ref, src_ref, packed_ref, meta_ref, tokens, stage, fill, sems):
    core = lax.rem(lax.axis_index("tp"), 2)
    pairs = src_ref.shape[0]
    step = pairs // 4
    copies = []
    for i in range(4):
        copies.append(
            pltpu.make_async_copy(
                src_ref.at[pl.ds(i * step, step), :, pl.ds(pl.multiple_of(core * HALF, HALF), HALF)],
                tokens.at[pl.ds(i * step, step)],
                sems.at[i],
            )
        )
        copies[-1].start()

    def clear(u, _):
        fill[u] = 0
        return 0

    lax.fori_loop(0, SLOTS, clear, 0)
    meta_ref[...] = jnp.zeros_like(meta_ref)
    lane = lax.broadcasted_iota(jnp.int32, (1, 128), 1)

    def place(i, _):
        u = tenant_ref[i]
        n = length_ref[i]
        start = fill[u]
        fill[u] = start + n
        code = start * 256 + start + n
        inside = ((lane % CAP) >= start) & ((lane % CAP) < start + n)
        meta_ref[u] = jnp.where(inside, code, meta_ref[u])
        for c in range(4):
            piece = tokens[i, :, c * 128 : c * 128 + 128].astype(jnp.float32)
            stage[u, c, pl.ds(start, CAP), :] = piece
        return 0

    for i in range(4):
        copies[i].wait()
        lax.fori_loop(i * step, (i + 1) * step, place, 0)
    row = lax.broadcasted_iota(jnp.int32, (CAP, 128), 0)

    def finish(u, _):
        for c in range(4):
            rows = jnp.where(row < fill[u], stage[u, c, 0:CAP, :], 0.0).astype(jnp.bfloat16)
            packed_ref[u, :, c * 128 : c * 128 + 128] = rows
        return 0

    lax.fori_loop(0, SLOTS, finish, 0)


def pack(tenant, length, tokens):
    pairs = tokens.shape[0]
    smem = pl.BlockSpec(memory_space=pltpu.SMEM)
    vmem = pl.BlockSpec(memory_space=pltpu.VMEM)
    return pl.pallas_call(
        pack_kernel,
        out_shape=(
            jax.ShapeDtypeStruct((SLOTS, CAP, HALF), jnp.bfloat16),
            jax.ShapeDtypeStruct((SLOTS, 1, 128), jnp.int32),
        ),
        in_specs=[smem, smem, pl.BlockSpec(memory_space=pl.ANY)],
        out_specs=(vmem, vmem),
        scratch_shapes=[
            pltpu.VMEM((pairs, CAP, HALF), jnp.bfloat16),
            pltpu.VMEM((SLOTS, 4, 2 * CAP, 128), jnp.float32),
            pltpu.SMEM((SLOTS,), jnp.int32),
            pltpu.SemaphoreType.DMA((4,)),
        ],
        compiler_params=pltpu.CompilerParams(vmem_limit_bytes=40 * 1024 * 1024),
        name="pack",
    )(tenant, length, tokens)


def here():
    t = lax.axis_index("tenant")
    p = lax.axis_index("tp")
    return t // 8, (t // 2) % 4, t % 2, p // 2, p % 2


def device(z, x, lo, hi, core):
    return ((z % 4) * 8 + (x % 4) * 2 + lo % 2, (hi % 2) * 2 + core % 2)


def shift_of(pos):
    g = pos // 4
    a = (pos // 2) % 2
    b = pos % 2
    dz = g % 2 + 2 * a
    dx = (g // 2 + b) % 4
    return dz, dx, b


def layer_kernel(
    packed_ref, meta_ref, gain_ref, bias_ref, wq_hbm, wk_hbm, wv_hbm, wo_hbm, out_ref,
    wq, wk, wv, wo, arr, codes, normed, query, key, value, context, part,
    scores, probs, totals, keep, pair_out, pair_in, mate_out, mate_in, far_out, far_in, mine,
    wsem, tok_s, tok_r, meta_s, meta_r, fwd_s, fwd_r,
    pair_s, pair_r, mate_s, mate_r, far_s, far_r,
):
    z, x, lo, hi, core = here()
    tenant = lax.axis_index("tenant")
    partner = device(z, x, lo, hi, core + 1)

    def peer(pos):
        dz, dx, dl = shift_of(pos)
        return device(z + dz, x + dx, lo + dl, hi + dl * ((dz + dx) % 2), core)

    weights = [
        pltpu.make_async_copy(src.at[0], dst, wsem.at[i])
        for i, (src, dst) in enumerate(((wq_hbm, wq), (wk_hbm, wk), (wv_hbm, wv), (wo_hbm, wo)))
    ]
    for copy in weights:
        copy.start()

    barrier = pltpu.get_barrier_semaphore()

    def greet(pos, _):
        pl.semaphore_signal(barrier, inc=1, device_id=peer(pos), device_id_type=MESH)
        return 0

    lax.fori_loop(1, SLOTS, greet, 0)
    pl.semaphore_signal(barrier, inc=1, device_id=partner, device_id_type=MESH)
    for c in range(2):
        pl.semaphore_signal(
            barrier, inc=1, device_id=device(z, x, lo, hi + 1, c), device_id_type=MESH
        )
    pl.semaphore_wait(barrier, SLOTS + 2)

    def token_copy(pos):
        target = peer(pos)
        return pltpu.make_async_remote_copy(
            packed_ref.at[target[0]], arr.at[core, pos], tok_s.at[pos], tok_r.at[pos],
            device_id=target, device_id_type=MESH,
        )

    def meta_copy(pos):
        target = peer(pos)
        return pltpu.make_async_remote_copy(
            meta_ref.at[target[0]], codes.at[pos], meta_s.at[pos], meta_r.at[pos],
            device_id=target, device_id_type=MESH,
        )

    def forward_copy(pos):
        return pltpu.make_async_remote_copy(
            arr.at[core, pos], arr.at[core, pos], fwd_s.at[pos], fwd_r.at[pos],
            device_id=partner, device_id_type=MESH,
        )

    own_forward = pltpu.make_async_remote_copy(
        packed_ref.at[tenant], arr.at[core, 0], fwd_s.at[0], fwd_r.at[0],
        device_id=partner, device_id_type=MESH,
    )
    def wait_partner(pos):
        pltpu.make_async_remote_copy(
            arr.at[1 - core, pos], arr.at[1 - core, pos], fwd_s.at[pos], fwd_r.at[pos],
            device_id=partner, device_id_type=MESH,
        ).wait_recv()

    own_forward.start()

    def send(pos, _):
        meta_copy(pos).start()
        token_copy(pos).start()
        return 0

    lax.fori_loop(1, SLOTS, send, 0)
    arr[core, 0] = packed_ref[tenant]
    codes[0] = meta_ref[tenant]

    def receive(pos):
        token_copy(pos).wait_recv()
        meta_copy(pos).wait_recv()
        forward_copy(pos).start()

    for pos in range(1, 4):
        receive(pos)

    def planes(g):
        first = (z + 4 - g % 2) % 4
        other = (first + 2) % 4
        first_far = jnp.where(first // 2 != hi, 1, 0)
        far_pair = 1 - first_far
        far_plane = jnp.where(first_far == 1, first, other)
        near_plane = jnp.where(first_far == 1, other, first)
        return far_pair, far_plane, near_plane

    def pair_copy(g):
        return pltpu.make_async_remote_copy(
            pair_out.at[g], pair_in.at[g], pair_s.at[g], pair_r.at[g],
            device_id=partner, device_id_type=MESH,
        )

    def mate_copy(q):
        return pltpu.make_async_remote_copy(
            mate_out.at[q], mate_in.at[q], mate_s.at[q], mate_r.at[q],
            device_id=partner, device_id_type=MESH,
        )

    def far_copy(g):
        _, far_plane, _ = planes(g)
        return pltpu.make_async_remote_copy(
            far_out.at[g], far_in.at[core, g // 2], far_s.at[g], far_r.at[core, g // 2],
            device_id=device(z, x, lo, hi + 1, far_plane), device_id_type=MESH,
        )

    def finish_pair(g):
        pair_copy(g).wait_recv()
        total = keep[g % 2] + pair_in[g].astype(jnp.float32)
        far_out[g] = total.astype(jnp.bfloat16)
        far_copy(g).start()

    row = lax.broadcasted_iota(jnp.int32, (CAP, 128), 0)
    west = lax.broadcasted_iota(jnp.int32, (CAP, 128), 1) < CAP
    blank = jnp.zeros((CAP, DK), jnp.bfloat16)
    ones = (
        (lax.broadcasted_iota(jnp.int32, (128, 256), 0) < CAP)
        == (lax.broadcasted_iota(jnp.int32, (128, 256), 1) < DK)
    ).astype(jnp.bfloat16)

    def group(g, _):
        base = g * 4
        for i in range(4):
            wait_partner(base + i)
        left = arr[0, pl.ds(base, 4)].reshape(256, HALF).astype(jnp.float32)
        right = arr[1, pl.ds(base, 4)].reshape(256, HALF).astype(jnp.float32)
        mean = (
            jnp.sum(left * left, axis=-1, keepdims=True)
            + jnp.sum(right * right, axis=-1, keepdims=True)
        ) / D
        scale = lax.rsqrt(mean + EPS)
        normed[:, 0:HALF] = (left * scale * gain_ref[:, 0:HALF]).astype(jnp.bfloat16)
        normed[:, HALF:D] = (right * scale * gain_ref[:, HALF:D]).astype(jnp.bfloat16)

        @pl.when(g == 0)
        def _():
            for copy in weights:
                copy.wait()

        rows = normed[...]
        query[...] = jnp.dot(rows, wq[...], preferred_element_type=jnp.float32).astype(jnp.bfloat16)
        key[...] = jnp.dot(rows, wk[...], preferred_element_type=jnp.float32).astype(jnp.bfloat16)
        value[...] = jnp.dot(rows, wv[...], preferred_element_type=jnp.float32).astype(jnp.bfloat16)

        @pl.when(g > 0)
        def _():
            finish_pair(g - 1)

        @pl.when(g < GROUPS - 1)
        def _():
            for i in range(4):
                receive(base + 4 + i)

        for block in range(2):
            code = jnp.where(west[0:1], codes[base + 2 * block], codes[base + 2 * block + 1])
            allowed = (row >= code // 256) & (row < code % 256)
            top = slice(block * 128, block * 128 + CAP)
            low = slice(block * 128 + CAP, block * 128 + 128)
            for h in range(HEADS):
                lanes = slice(h * DK, h * DK + DK)
                both = jnp.concatenate([query[top, lanes], query[low, lanes]], axis=1)
                keys = jnp.concatenate(
                    [
                        jnp.concatenate([key[top, lanes], blank], axis=1),
                        jnp.concatenate([blank, key[low, lanes]], axis=1),
                    ],
                    axis=0,
                )
                s = lax.dot_general(
                    both, keys, (((1,), (1,)), ((), ())), preferred_element_type=jnp.float32
                )
                scores[block, h] = jnp.where(allowed, s + bias_ref[h], NEG)
        for block in range(2):
            for h in range(HEADS):
                s = scores[block, h]
                first = jnp.max(jnp.where(west, s, NEG), axis=-1, keepdims=True)
                second = jnp.max(jnp.where(west, NEG, s), axis=-1, keepdims=True)
                peak = jnp.maximum(jnp.where(west, first, second), 0.5 * NEG)
                probs[block, h] = jnp.exp(s - peak).astype(jnp.bfloat16)
        for block in range(2):
            top = slice(block * 128, block * 128 + CAP)
            low = slice(block * 128 + CAP, block * 128 + 128)
            sums = jnp.dot(
                probs[block].reshape(HEADS * CAP, 128), ones, preferred_element_type=jnp.float32
            )
            totals[block] = (1.0 / jnp.maximum(sums, 0.5)).reshape(HEADS, CAP, 256)
            for h in range(HEADS):
                lanes = slice(h * DK, h * DK + DK)
                values = jnp.concatenate(
                    [
                        jnp.concatenate([value[top, lanes], blank], axis=1),
                        jnp.concatenate([blank, value[low, lanes]], axis=1),
                    ],
                    axis=0,
                )
                ctx = jnp.dot(probs[block, h], values, preferred_element_type=jnp.float32)
                ctx = (ctx * totals[block, h]).astype(jnp.bfloat16)
                context[top, lanes] = ctx[:, 0:DK]
                context[low, lanes] = ctx[:, DK : 2 * DK]

        part[...] = jnp.dot(context[...], wo[...], preferred_element_type=jnp.float32)
        far_pair, _, near_plane = planes(g)
        far_rows = pl.ds(pl.multiple_of(far_pair * 128, 128), 128)
        near_rows = pl.ds(pl.multiple_of((1 - far_pair) * 128, 128), 128)
        own_cols = pl.ds(pl.multiple_of(core * HALF, HALF), HALF)
        other_cols = pl.ds(pl.multiple_of((1 - core) * HALF, HALF), HALF)
        pair_out[g] = part[far_rows, other_cols].astype(jnp.bfloat16)
        pair_copy(g).start()
        keep[g % 2] = part[far_rows, own_cols]

        @pl.when(near_plane % 2 == core)
        def _():
            mine[g // 2] = part[near_rows, :]

        @pl.when(near_plane % 2 != core)
        def _():
            mate_out[g // 2] = part[near_rows, :].astype(jnp.bfloat16)
            mate_copy(g // 2).start()

        return 0

    lax.fori_loop(0, GROUPS, group, 0)
    finish_pair(GROUPS - 1)

    plane = hi * 2 + core
    parity = (z + plane) % 2

    def combine(q, _):
        g = 2 * q + parity
        far_pair, _, _ = planes(g)
        near_pair = 1 - far_pair
        mate_copy(q).wait_recv()
        for c in range(2):
            pltpu.make_async_remote_copy(
                far_in.at[c, q], far_in.at[c, q], far_s.at[q], far_r.at[c, q],
                device_id=partner, device_id_type=MESH,
            ).wait_recv()
        for b in range(2):
            pos = g * 4 + near_pair * 2 + b
            src_slot = ((x + 8 - q - b) % 4) * 2 + (lo + b) % 2
            span = slice(b * CAP, b * CAP + CAP)
            for c in range(2):
                cols = slice(c * HALF, c * HALF + HALF)
                total = (
                    mine[q, span, cols]
                    + mate_in[q, span, cols].astype(jnp.float32)
                    + far_in[c, q, span, :].astype(jnp.float32)
                    + arr[c, pos].astype(jnp.float32)
                )
                out_ref[src_slot, :, cols] = total.astype(jnp.bfloat16)
        return 0

    lax.fori_loop(0, 4, combine, 0)

    def drain(pos, _):
        token_copy(pos).wait_send()
        meta_copy(pos).wait_send()
        forward_copy(pos).wait_send()
        return 0

    own_forward.wait_send()
    lax.fori_loop(1, SLOTS, drain, 0)

    def drain_groups(g, _):
        pair_copy(g).wait_send()
        far_copy(g).wait_send()
        return 0

    lax.fori_loop(0, GROUPS, drain_groups, 0)

    def drain_mates(q, _):
        mate_copy(q).wait_send()
        return 0

    lax.fori_loop(0, 4, drain_mates, 0)


def layer(packed, meta, gain, bias, wq, wk, wv, wo):
    vmem = pl.BlockSpec(memory_space=pltpu.VMEM)
    anywhere = pl.BlockSpec(memory_space=pl.ANY)
    bf, f32 = jnp.bfloat16, jnp.float32
    dma = pltpu.SemaphoreType.DMA
    return pl.pallas_call(
        layer_kernel,
        out_shape=jax.ShapeDtypeStruct((8, CAP, D), bf),
        in_specs=[vmem] * 4 + [anywhere] * 4,
        out_specs=vmem,
        scratch_shapes=[pltpu.VMEM((D, D), bf)] * 4
        + [
            pltpu.VMEM((2, SLOTS, CAP, HALF), bf),
            pltpu.VMEM((SLOTS, 1, 128), jnp.int32),
        ]
        + [pltpu.VMEM((256, D), bf)] * 5
        + [
            pltpu.VMEM((256, D), f32),
            pltpu.VMEM((2, HEADS, CAP, 128), f32),
            pltpu.VMEM((2, HEADS, CAP, 128), bf),
            pltpu.VMEM((2, HEADS, CAP, 256), f32),
            pltpu.VMEM((2, 128, HALF), f32),
            pltpu.VMEM((GROUPS, 128, HALF), bf),
            pltpu.VMEM((GROUPS, 128, HALF), bf),
            pltpu.VMEM((4, 128, D), bf),
            pltpu.VMEM((4, 128, D), bf),
            pltpu.VMEM((GROUPS, 128, HALF), bf),
            pltpu.VMEM((2, 4, 128, HALF), bf),
            pltpu.VMEM((4, 128, D), f32),
            dma((4,)), dma((SLOTS,)), dma((SLOTS,)), dma((SLOTS,)), dma((SLOTS,)),
            dma((SLOTS,)), dma((SLOTS,)),
            dma((GROUPS,)), dma((GROUPS,)), dma((4,)), dma((4,)), dma((GROUPS,)), dma((2, 4)),
        ],
        compiler_params=pltpu.CompilerParams(
            collective_id=0, has_side_effects=True, vmem_limit_bytes=56 * 1024 * 1024
        ),
        name="layer",
    )(packed, meta, gain, bias, wq, wk, wv, wo)


def per_device(
    src_tokens, pair_tenant, pair_length, norm_gain, w_query, w_key, w_value, w_out, rel_bias
):
    packed, meta = pack(pair_tenant, pair_length, src_tokens)
    bias = position_bias(rel_bias[0])
    out = layer(packed, meta, norm_gain, bias, w_query, w_key, w_value, w_out)
    return out.reshape(8 * CAP, D)


def solution(mesh):
    in_specs = (
        P("tenant", None, None),
        P("tenant"),
        P("tenant"),
        P("tenant", None),
        P("tenant", None, "tp"),
        P("tenant", None, "tp"),
        P("tenant", None, "tp"),
        P("tenant", "tp", None),
        P("tenant", None, "tp"),
    )
    out_specs = P(("tenant", "tp"), None)
    return jax.shard_map(
        per_device, mesh=mesh, in_specs=in_specs, out_specs=out_specs, check_vma=False
    )
```

```python
import functools
import math

import jax
import jax.numpy as jnp
import numpy as np
from jax import lax
from jax.experimental import pallas as pl
from jax.experimental.pallas import tpu as pltpu
from jax.sharding import PartitionSpec as P

MESH = pl.DeviceIdType.MESH
CAP = 64
D = 1024
HALF = 512
SLOTS = 32
GROUPS = 8
HEADS = 8
DK = 128
NEG = -1e30
EPS = 1e-6
BUCKETS = 32
SELF = 16


def bucket_limits():
    distance = np.arange(8, CAP)
    steps = np.floor(np.log(distance / 8) / math.log(16.0) * 8).astype(np.int32)
    steps = np.minimum(steps, 7)
    return [int(distance[steps >= n][0]) for n in range(1, int(steps.max()) + 1)]


def here():
    t = lax.axis_index("tenant")
    p = lax.axis_index("tp")
    return t // 8, (t // 2) % 4, t % 2, p // 2, p % 2


def device(z, x, lo, hi, core):
    return ((z % 4) * 8 + (x % 4) * 2 + lo % 2, (hi % 2) * 2 + core % 2)


def shift_of(pos):
    g = pos // 4
    a = (pos // 2) % 2
    b = pos % 2
    odd_z = g % 2
    odd_x = (g // 2) % 2
    dl = 1 - g // 4
    flip = dl * jnp.where(odd_z == odd_x, (a + b) % 2, jnp.where(odd_z == 1, b, a))
    return odd_z + 2 * a, odd_x + 2 * b, dl, flip


def layer_kernel(
    tenant_ref, length_ref, table_ref, gain_ref, src_hbm, wq_hbm, wk_hbm, wv_hbm, wo_hbm, out_ref,
    wq, wk, wv, wo, tokens, pick, packed, spots, meta, bias,
    arr, codes, normed, query, key, value, context, part,
    scores, probs, totals, keep, pair_out, pair_in, mate_out, mate_in, far_out, far_in, mine,
    ssem, wsem, tok_s, tok_r, meta_s, meta_r, fwd_s, fwd_r,
    pair_s, pair_r, mate_s, mate_r, far_s, far_r,
):
    z, x, lo, hi, core = here()
    tenant = lax.axis_index("tenant")
    partner = device(z, x, lo, hi, core + 1)
    pairs = src_hbm.shape[0]
    chunks = pairs * CAP // 128

    def peer(pos):
        dz, dx, dl, flip = shift_of(pos)
        return device(z + dz, x + dx, lo + dl, hi + flip, core)

    source = pltpu.make_async_copy(
        src_hbm.at[:, :, pl.ds(pl.multiple_of(core * HALF, HALF), HALF)], tokens, ssem.at[0]
    )
    source.start()
    weights = [
        pltpu.make_async_copy(src.at[0], dst, wsem.at[i])
        for i, (src, dst) in enumerate(((wq_hbm, wq), (wk_hbm, wk), (wv_hbm, wv), (wo_hbm, wo)))
    ]
    for copy in weights:
        copy.start()

    barrier = pltpu.get_barrier_semaphore()

    def greet(pos, _):
        @pl.when(pos != SELF)
        def _():
            pl.semaphore_signal(barrier, inc=1, device_id=peer(pos), device_id_type=MESH)

        return 0

    lax.fori_loop(0, SLOTS, greet, 0)
    pl.semaphore_signal(barrier, inc=1, device_id=partner, device_id_type=MESH)
    for c in range(2):
        pl.semaphore_signal(
            barrier, inc=1, device_id=device(z, x, lo, hi + 1, c), device_id_type=MESH
        )

    lane = lax.broadcasted_iota(jnp.int32, (chunks, 128), 1)
    pair_of = lax.broadcasted_iota(jnp.int32, (chunks, 128), 0) * 2 + lane // CAP
    place = lane % CAP
    slot_of = lax.broadcasted_iota(jnp.int32, (SLOTS, 128), 0)
    slot_row = lax.broadcasted_iota(jnp.int32, (SLOTS, 128), 1) % CAP

    def spread(j, carry):
        whose, count = carry
        here_now = pair_of == j
        return jnp.where(here_now, tenant_ref[j], whose), jnp.where(here_now, length_ref[j], count)

    nothing = jnp.zeros((chunks, 128), jnp.int32)
    whose, count = lax.fori_loop(0, pairs, spread, (nothing, nothing))

    def stack(j, carry):
        offset, fill, code = carry
        who, size = tenant_ref[j], length_ref[j]
        offset = offset + jnp.where((whose == who) & (pair_of > j), size, 0)
        hit = slot_of == who
        inside = hit & (slot_row >= fill) & (slot_row < fill + size)
        code = jnp.where(inside, fill * 257 + size, code)
        return offset, jnp.where(hit, fill + size, fill), code

    empty = jnp.zeros((SLOTS, 128), jnp.int32)
    offset, _, code = lax.fori_loop(0, pairs, stack, (nothing, empty, empty))
    spots[...] = jnp.where(place < count, whose * CAP + offset + place, -1)
    for u in range(SLOTS):
        meta[u] = code[u : u + 1, :]

    row = lax.broadcasted_iota(jnp.int32, (CAP, 128), 0)
    west = lax.broadcasted_iota(jnp.int32, (CAP, 128), 1) < CAP

    def pack(g):
        slots = [peer(g * 4 + s)[0] * CAP for s in range(4)]
        for m in range(chunks):
            spot = spots[m : m + 1, :]
            for s in range(4):
                pick[s * CAP : s * CAP + CAP, m * 128 : m * 128 + 128] = jnp.where(
                    row == spot - slots[s], 1.0, 0.0
                ).astype(jnp.bfloat16)
        rows = jnp.dot(
            pick[...], tokens[...].reshape(pairs * CAP, HALF), preferred_element_type=jnp.float32
        )
        packed[pl.ds(g * 4, 4)] = rows.astype(jnp.bfloat16).reshape(4, CAP, HALF)

    def token_copy(pos):
        target = peer(pos)
        return pltpu.make_async_remote_copy(
            packed.at[pos], arr.at[core, pos], tok_s.at[pos], tok_r.at[pos],
            device_id=target, device_id_type=MESH,
        )

    def meta_copy(pos):
        target = peer(pos)
        return pltpu.make_async_remote_copy(
            meta.at[target[0]], codes.at[pos], meta_s.at[pos], meta_r.at[pos],
            device_id=target, device_id_type=MESH,
        )

    def forward_copy(pos):
        return pltpu.make_async_remote_copy(
            arr.at[core, pos], arr.at[core, pos], fwd_s.at[pos], fwd_r.at[pos],
            device_id=partner, device_id_type=MESH,
        )

    own_forward = pltpu.make_async_remote_copy(
        packed.at[SELF], arr.at[core, SELF], fwd_s.at[SELF], fwd_r.at[SELF],
        device_id=partner, device_id_type=MESH,
    )

    def wait_partner(pos):
        pltpu.make_async_remote_copy(
            arr.at[1 - core, pos], arr.at[1 - core, pos], fwd_s.at[pos], fwd_r.at[pos],
            device_id=partner, device_id_type=MESH,
        ).wait_recv()

    def send(pos):
        @pl.when(pos != SELF)
        def _():
            meta_copy(pos).start()
            token_copy(pos).start()

    def send_group(g):
        for i in range(4):
            send(g * 4 + i)

    source.wait()
    pack(0)
    pl.semaphore_wait(barrier, SLOTS + 2)

    def pack_and_send(g, _):
        pack(g)
        send_group(g - 1)
        return 0

    lax.fori_loop(1, GROUPS, pack_and_send, 0)
    send_group(GROUPS - 1)
    own_forward.start()
    arr[core, SELF] = packed[SELF]
    codes[SELF] = meta[tenant]

    ahead = lax.broadcasted_iota(jnp.int32, (CAP, 128), 1) % CAP - row
    distance = jnp.abs(ahead)
    bucket = jnp.where(distance < 8, distance, 8)
    for limit in bucket_limits():
        bucket = bucket + jnp.where(distance >= limit, 1, 0)
    bucket = bucket + jnp.where(ahead > 0, 16, 0)

    def expand(h, _):
        total = jnp.zeros((CAP, 128), jnp.float32)
        for k in range(BUCKETS):
            total = jnp.where(bucket == k, table_ref[h, k], total)
        bias[h] = total
        return 0

    lax.fori_loop(0, HEADS, expand, 0)

    def receive(pos):
        @pl.when(pos != SELF)
        def _():
            token_copy(pos).wait_recv()
            meta_copy(pos).wait_recv()
            forward_copy(pos).start()

    for pos in range(4):
        receive(pos)

    def planes(g):
        first = (z + 4 - g % 2) % 4
        other = (first + 2) % 4
        first_far = jnp.where(first // 2 != hi, 1, 0)
        far_pair = 1 - first_far
        far_plane = jnp.where(first_far == 1, first, other)
        near_plane = jnp.where(first_far == 1, other, first)
        return far_pair, far_plane, near_plane

    def pair_copy(g):
        return pltpu.make_async_remote_copy(
            pair_out.at[g], pair_in.at[g], pair_s.at[g], pair_r.at[g],
            device_id=partner, device_id_type=MESH,
        )

    def mate_copy(q):
        return pltpu.make_async_remote_copy(
            mate_out.at[q], mate_in.at[q], mate_s.at[q], mate_r.at[q],
            device_id=partner, device_id_type=MESH,
        )

    def far_copy(g):
        _, far_plane, _ = planes(g)
        return pltpu.make_async_remote_copy(
            far_out.at[g], far_in.at[core, g // 2], far_s.at[g], far_r.at[core, g // 2],
            device_id=device(z, x, lo, hi + 1, far_plane), device_id_type=MESH,
        )

    def finish_pair(g):
        pair_copy(g).wait_recv()
        total = keep[g % 2] + pair_in[g].astype(jnp.float32)
        far_out[g] = total.astype(jnp.bfloat16)
        far_copy(g).start()

    blank = jnp.zeros((CAP, DK), jnp.bfloat16)
    ones = (
        (lax.broadcasted_iota(jnp.int32, (128, 256), 0) < CAP)
        == (lax.broadcasted_iota(jnp.int32, (128, 256), 1) < DK)
    ).astype(jnp.bfloat16)

    def group(g, _):
        base = g * 4
        for i in range(4):
            wait_partner(base + i)
        left = arr[0, pl.ds(base, 4)].reshape(256, HALF).astype(jnp.float32)
        right = arr[1, pl.ds(base, 4)].reshape(256, HALF).astype(jnp.float32)
        mean = (
            jnp.sum(left * left, axis=-1, keepdims=True)
            + jnp.sum(right * right, axis=-1, keepdims=True)
        ) / D
        scale = lax.rsqrt(mean + EPS)
        normed[:, 0:HALF] = (left * scale * gain_ref[:, 0:HALF]).astype(jnp.bfloat16)
        normed[:, HALF:D] = (right * scale * gain_ref[:, HALF:D]).astype(jnp.bfloat16)

        @pl.when(g == 0)
        def _():
            for copy in weights:
                copy.wait()

        rows = normed[...]
        query[...] = jnp.dot(rows, wq[...], preferred_element_type=jnp.float32).astype(jnp.bfloat16)
        key[...] = jnp.dot(rows, wk[...], preferred_element_type=jnp.float32).astype(jnp.bfloat16)
        value[...] = jnp.dot(rows, wv[...], preferred_element_type=jnp.float32).astype(jnp.bfloat16)

        @pl.when(g > 0)
        def _():
            finish_pair(g - 1)

        @pl.when(g < GROUPS - 1)
        def _():
            for i in range(4):
                receive(base + 4 + i)

        for block in range(2):
            code = jnp.where(west[0:1], codes[base + 2 * block], codes[base + 2 * block + 1])
            allowed = (row >= code // 256) & (row < code % 256)
            top = slice(block * 128, block * 128 + CAP)
            low = slice(block * 128 + CAP, block * 128 + 128)
            for h in range(HEADS):
                lanes = slice(h * DK, h * DK + DK)
                both = jnp.concatenate([query[top, lanes], query[low, lanes]], axis=1)
                keys = jnp.concatenate(
                    [
                        jnp.concatenate([key[top, lanes], blank], axis=1),
                        jnp.concatenate([blank, key[low, lanes]], axis=1),
                    ],
                    axis=0,
                )
                s = lax.dot_general(
                    both, keys, (((1,), (1,)), ((), ())), preferred_element_type=jnp.float32
                )
                scores[block, h] = jnp.where(allowed, s + bias[h], NEG)
        for block in range(2):
            for h in range(HEADS):
                s = scores[block, h]
                first = jnp.max(jnp.where(west, s, NEG), axis=-1, keepdims=True)
                second = jnp.max(jnp.where(west, NEG, s), axis=-1, keepdims=True)
                peak = jnp.maximum(jnp.where(west, first, second), 0.5 * NEG)
                probs[block, h] = jnp.exp(s - peak).astype(jnp.bfloat16)
        for block in range(2):
            top = slice(block * 128, block * 128 + CAP)
            low = slice(block * 128 + CAP, block * 128 + 128)
            sums = jnp.dot(
                probs[block].reshape(HEADS * CAP, 128), ones, preferred_element_type=jnp.float32
            )
            totals[block] = (1.0 / jnp.maximum(sums, 0.5)).reshape(HEADS, CAP, 256)
            for h in range(HEADS):
                lanes = slice(h * DK, h * DK + DK)
                values = jnp.concatenate(
                    [
                        jnp.concatenate([value[top, lanes], blank], axis=1),
                        jnp.concatenate([blank, value[low, lanes]], axis=1),
                    ],
                    axis=0,
                )
                ctx = jnp.dot(probs[block, h], values, preferred_element_type=jnp.float32)
                ctx = (ctx * totals[block, h]).astype(jnp.bfloat16)
                context[top, lanes] = ctx[:, 0:DK]
                context[low, lanes] = ctx[:, DK : 2 * DK]

        part[...] = jnp.dot(context[...], wo[...], preferred_element_type=jnp.float32)
        far_pair, _, near_plane = planes(g)
        far_rows = pl.ds(pl.multiple_of(far_pair * 128, 128), 128)
        near_rows = pl.ds(pl.multiple_of((1 - far_pair) * 128, 128), 128)
        own_cols = pl.ds(pl.multiple_of(core * HALF, HALF), HALF)
        other_cols = pl.ds(pl.multiple_of((1 - core) * HALF, HALF), HALF)
        pair_out[g] = part[far_rows, other_cols].astype(jnp.bfloat16)
        pair_copy(g).start()
        keep[g % 2] = part[far_rows, own_cols]

        @pl.when(near_plane % 2 == core)
        def _():
            mine[g // 2] = part[near_rows, :]

        @pl.when(near_plane % 2 != core)
        def _():
            mate_out[g // 2] = part[near_rows, :].astype(jnp.bfloat16)
            mate_copy(g // 2).start()

        return 0

    lax.fori_loop(0, GROUPS, group, 0)
    finish_pair(GROUPS - 1)

    plane = hi * 2 + core
    parity = (z + plane) % 2

    def combine(q, _):
        g = 2 * q + parity
        far_pair, _, _ = planes(g)
        near_pair = 1 - far_pair
        mate_copy(q).wait_recv()
        for c in range(2):
            pltpu.make_async_remote_copy(
                far_in.at[c, q], far_in.at[c, q], far_s.at[q], far_r.at[c, q],
                device_id=partner, device_id_type=MESH,
            ).wait_recv()
        for b in range(2):
            pos = g * 4 + near_pair * 2 + b
            _, dx, dl, _ = shift_of(pos)
            src_slot = ((x + 4 - dx) % 4) * 2 + (lo + dl) % 2
            span = slice(b * CAP, b * CAP + CAP)
            for c in range(2):
                cols = slice(c * HALF, c * HALF + HALF)
                total = (
                    mine[q, span, cols]
                    + mate_in[q, span, cols].astype(jnp.float32)
                    + far_in[c, q, span, :].astype(jnp.float32)
                    + arr[c, pos].astype(jnp.float32)
                )
                out_ref[src_slot, :, cols] = total.astype(jnp.bfloat16)
        return 0

    lax.fori_loop(0, 4, combine, 0)

    def drain(pos, _):
        @pl.when(pos != SELF)
        def _():
            token_copy(pos).wait_send()
            meta_copy(pos).wait_send()
            forward_copy(pos).wait_send()

        return 0

    own_forward.wait_send()
    lax.fori_loop(0, SLOTS, drain, 0)

    def drain_groups(g, _):
        pair_copy(g).wait_send()
        far_copy(g).wait_send()
        return 0

    lax.fori_loop(0, GROUPS, drain_groups, 0)

    def drain_mates(q, _):
        mate_copy(q).wait_send()
        return 0

    lax.fori_loop(0, 4, drain_mates, 0)


def layer(tenant, length, table, gain, tokens, wq, wk, wv, wo):
    pairs = tokens.shape[0]
    smem = pl.BlockSpec(memory_space=pltpu.SMEM)
    vmem = pl.BlockSpec(memory_space=pltpu.VMEM)
    anywhere = pl.BlockSpec(memory_space=pl.ANY)
    bf, f32 = jnp.bfloat16, jnp.float32
    dma = pltpu.SemaphoreType.DMA
    return pl.pallas_call(
        layer_kernel,
        out_shape=jax.ShapeDtypeStruct((8, CAP, D), bf),
        in_specs=[smem] * 3 + [vmem] + [anywhere] * 5,
        out_specs=vmem,
        scratch_shapes=[pltpu.VMEM((D, D), bf)] * 4
        + [
            pltpu.VMEM((pairs, CAP, HALF), bf),
            pltpu.VMEM((256, pairs * CAP), bf),
            pltpu.VMEM((SLOTS, CAP, HALF), bf),
            pltpu.VMEM((pairs * CAP // 128, 128), jnp.int32),
            pltpu.VMEM((SLOTS, 1, 128), jnp.int32),
            pltpu.VMEM((HEADS, CAP, 128), f32),
            pltpu.VMEM((2, SLOTS, CAP, HALF), bf),
            pltpu.VMEM((SLOTS, 1, 128), jnp.int32),
        ]
        + [pltpu.VMEM((256, D), bf)] * 5
        + [
            pltpu.VMEM((256, D), f32),
            pltpu.VMEM((2, HEADS, CAP, 128), f32),
            pltpu.VMEM((2, HEADS, CAP, 128), bf),
            pltpu.VMEM((2, HEADS, CAP, 256), f32),
            pltpu.VMEM((2, 128, HALF), f32),
            pltpu.VMEM((GROUPS, 128, HALF), bf),
            pltpu.VMEM((GROUPS, 128, HALF), bf),
            pltpu.VMEM((4, 128, D), bf),
            pltpu.VMEM((4, 128, D), bf),
            pltpu.VMEM((GROUPS, 128, HALF), bf),
            pltpu.VMEM((2, 4, 128, HALF), bf),
            pltpu.VMEM((4, 128, D), f32),
            dma((1,)), dma((4,)), dma((SLOTS,)), dma((SLOTS,)), dma((SLOTS,)), dma((SLOTS,)),
            dma((SLOTS,)), dma((SLOTS,)),
            dma((GROUPS,)), dma((GROUPS,)), dma((4,)), dma((4,)), dma((GROUPS,)), dma((2, 4)),
        ],
        compiler_params=pltpu.CompilerParams(
            collective_id=0, has_side_effects=True, vmem_limit_bytes=67_043_328
        ),
        name="layer",
    )(tenant, length, table, gain, tokens, wq, wk, wv, wo)


def per_device(
    src_tokens, pair_tenant, pair_length, norm_gain, w_query, w_key, w_value, w_out, rel_bias
):
    table = jnp.transpose(rel_bias[0])
    out = layer(
        pair_tenant, pair_length, table, norm_gain, src_tokens, w_query, w_key, w_value, w_out
    )
    return out.reshape(8 * CAP, D)


def solution(mesh):
    in_specs = (
        P("tenant", None, None),
        P("tenant"),
        P("tenant"),
        P("tenant", None),
        P("tenant", None, "tp"),
        P("tenant", None, "tp"),
        P("tenant", None, "tp"),
        P("tenant", "tp", None),
        P("tenant", None, "tp"),
    )
    out_specs = P(("tenant", "tp"), None)
    return jax.shard_map(
        per_device, mesh=mesh, in_specs=in_specs, out_specs=out_specs, check_vma=False
    )
```

```python
import functools
import math

import jax
import jax.numpy as jnp
import numpy as np
from jax import lax
from jax.experimental import pallas as pl
from jax.experimental.pallas import tpu as pltpu
from jax.sharding import PartitionSpec as P

MESH = pl.DeviceIdType.MESH
CAP = 64
D = 1024
HALF = 512
SLOTS = 32
GROUPS = 8
HEADS = 8
DK = 128
NEG = -1e30
EPS = 1e-6
BUCKETS = 32
SELF = 16


def bucket_limits():
    distance = np.arange(8, CAP)
    steps = np.floor(np.log(distance / 8) / math.log(16.0) * 8).astype(np.int32)
    steps = np.minimum(steps, 7)
    return [int(distance[steps >= n][0]) for n in range(1, int(steps.max()) + 1)]


def unrolled(count, body, carry):
    def steps(block, carry):
        for i in range(12):
            carry = body(block * 12 + i, carry)
        return carry

    return lax.fori_loop(0, count // 12, steps, carry)


def mod(a, b):
    return a % b if isinstance(a, int) else lax.rem(a, jnp.int32(b))


def div(a, b):
    return a // b if isinstance(a, int) else lax.div(a, jnp.int32(b))


def here():
    t = lax.axis_index("tenant")
    p = lax.axis_index("tp")
    return div(t, 8), mod(div(t, 2), 4), mod(t, 2), div(p, 2), mod(p, 2)


def device(z, x, lo, hi, core):
    return (mod(z, 4) * 8 + mod(x, 4) * 2 + mod(lo, 2), mod(hi, 2) * 2 + mod(core, 2))


def shift_of(pos):
    g = div(pos, 4)
    a = mod(div(pos, 2), 2)
    b = mod(pos, 2)
    odd_z = mod(g, 2)
    odd_x = mod(div(g, 2), 2)
    dl = 1 - div(g, 4)
    same = 1 - mod(odd_z + odd_x, 2)
    flip = dl * mod((same + (1 - same) * (1 - odd_z)) * a + (same + (1 - same) * odd_z) * b, 2)
    return odd_z + 2 * a, odd_x + 2 * b, dl, flip


def layer_kernel(
    tenant_ref, length_ref, table_ref, gain_ref, src_hbm, wq_hbm, wk_hbm, wv_hbm, wo_hbm, out_ref,
    wq, wk, wv, wo, tokens, pick, packed, spots, meta, bias,
    arr, codes, normed, query, key, value, context, part,
    scores, probs, totals, keep, pair_out, pair_in, mate_out, mate_in, far_out, far_in, mine,
    ssem, wsem, tok_s, tok_r, meta_s, meta_r, fwd_s, fwd_r,
    pair_s, pair_r, mate_s, mate_r, far_s, far_r,
):
    z, x, lo, hi, core = here()
    tenant = lax.axis_index("tenant")
    partner = device(z, x, lo, hi, core + 1)
    pairs = src_hbm.shape[0]
    chunks = pairs * CAP // 128

    def peer(pos):
        dz, dx, dl, flip = shift_of(pos)
        return device(z + dz, x + dx, lo + dl, hi + flip, core)

    source = pltpu.make_async_copy(
        src_hbm.at[:, :, pl.ds(pl.multiple_of(core * HALF, HALF), HALF)], tokens, ssem.at[0]
    )
    source.start()
    weights = [
        pltpu.make_async_copy(src.at[0], dst, wsem.at[i])
        for i, (src, dst) in enumerate(((wq_hbm, wq), (wk_hbm, wk), (wv_hbm, wv), (wo_hbm, wo)))
    ]
    for copy in weights:
        copy.start()

    barrier = pltpu.get_barrier_semaphore()

    for pos in range(SLOTS):
        if pos != SELF:
            pl.semaphore_signal(barrier, inc=1, device_id=peer(pos), device_id_type=MESH)
    pl.semaphore_signal(barrier, inc=1, device_id=partner, device_id_type=MESH)
    for c in range(2):
        pl.semaphore_signal(
            barrier, inc=1, device_id=device(z, x, lo, hi + 1, c), device_id_type=MESH
        )

    lane = lax.broadcasted_iota(jnp.int32, (chunks, 128), 1)
    pair_of = lax.broadcasted_iota(jnp.int32, (chunks, 128), 0) * 2 + lane // CAP
    place = lane % CAP
    slot_of = lax.broadcasted_iota(jnp.int32, (SLOTS, 128), 0)
    slot_row = lax.broadcasted_iota(jnp.int32, (SLOTS, 128), 1) % CAP

    def spread(j, carry):
        whose, count = carry
        here_now = pair_of == j
        return jnp.where(here_now, tenant_ref[j], whose), jnp.where(here_now, length_ref[j], count)

    nothing = jnp.zeros((chunks, 128), jnp.int32)
    whose, count = unrolled(pairs, spread, (nothing, nothing))

    def stack(j, carry):
        offset, fill, code = carry
        who, size = tenant_ref[j], length_ref[j]
        offset = offset + jnp.where((whose == who) & (pair_of > j), size, 0)
        hit = slot_of == who
        inside = hit & (slot_row >= fill) & (slot_row < fill + size)
        code = jnp.where(inside, fill * 257 + size, code)
        return offset, jnp.where(hit, fill + size, fill), code

    empty = jnp.zeros((SLOTS, 128), jnp.int32)
    offset, _, code = unrolled(pairs, stack, (nothing, empty, empty))
    spots[...] = jnp.where(place < count, whose * CAP + offset + place, -1)
    for u in range(SLOTS):
        meta[u] = code[u : u + 1, :]

    row = lax.broadcasted_iota(jnp.int32, (CAP, 128), 0)
    west = lax.broadcasted_iota(jnp.int32, (CAP, 128), 1) < CAP

    def pack(g):
        slots = [peer(g * 4 + s)[0] * CAP for s in range(4)]
        for m in range(chunks):
            spot = spots[m : m + 1, :]
            for s in range(4):
                pick[s * CAP : s * CAP + CAP, m * 128 : m * 128 + 128] = jnp.where(
                    row == spot - slots[s], 1.0, 0.0
                ).astype(jnp.bfloat16)
        rows = jnp.dot(
            pick[...], tokens[...].reshape(pairs * CAP, HALF), preferred_element_type=jnp.float32
        )
        packed[pl.ds(g * 4, 4)] = rows.astype(jnp.bfloat16).reshape(4, CAP, HALF)

    def token_copy(pos):
        target = peer(pos)
        return pltpu.make_async_remote_copy(
            packed.at[pos], arr.at[core, pos], tok_s.at[pos], tok_r.at[pos],
            device_id=target, device_id_type=MESH,
        )

    def meta_copy(pos):
        target = peer(pos)
        return pltpu.make_async_remote_copy(
            meta.at[target[0]], codes.at[pos], meta_s.at[pos], meta_r.at[pos],
            device_id=target, device_id_type=MESH,
        )

    def forward_copy(pos):
        return pltpu.make_async_remote_copy(
            arr.at[core, pos], arr.at[core, pos], fwd_s.at[pos], fwd_r.at[pos],
            device_id=partner, device_id_type=MESH,
        )

    own_forward = pltpu.make_async_remote_copy(
        packed.at[SELF], arr.at[core, SELF], fwd_s.at[SELF], fwd_r.at[SELF],
        device_id=partner, device_id_type=MESH,
    )

    def wait_partner(pos):
        pltpu.make_async_remote_copy(
            arr.at[1 - core, pos], arr.at[1 - core, pos], fwd_s.at[pos], fwd_r.at[pos],
            device_id=partner, device_id_type=MESH,
        ).wait_recv()

    def send(pos):
        @pl.when(pos != SELF)
        def _():
            meta_copy(pos).start()
            token_copy(pos).start()

    def send_group(g):
        for i in range(4):
            send(g * 4 + i)

    source.wait()
    pack(0)
    pl.semaphore_wait(barrier, SLOTS + 2)

    def pack_and_send(g, _):
        send_group(g - 1)
        pack(g)
        return 0

    lax.fori_loop(1, GROUPS, pack_and_send, 0)
    send_group(GROUPS - 1)
    own_forward.start()
    arr[core, SELF] = packed[SELF]
    codes[SELF] = meta[tenant]

    ahead = lax.broadcasted_iota(jnp.int32, (CAP, 128), 1) % CAP - row
    distance = jnp.abs(ahead)
    bucket = jnp.where(distance < 8, distance, 8)
    for limit in bucket_limits():
        bucket = bucket + jnp.where(distance >= limit, 1, 0)
    bucket = bucket + jnp.where(ahead > 0, 16, 0)

    def expand(h, _):
        total = jnp.zeros((CAP, 128), jnp.float32)
        for k in range(BUCKETS):
            total = jnp.where(bucket == k, table_ref[h, k], total)
        bias[h] = total
        return 0

    lax.fori_loop(0, HEADS, expand, 0)

    def receive(pos):
        @pl.when(pos != SELF)
        def _():
            token_copy(pos).wait_recv()
            meta_copy(pos).wait_recv()
            forward_copy(pos).start()

    for pos in range(4):
        receive(pos)

    def planes(g):
        first = (z + 4 - g % 2) % 4
        other = (first + 2) % 4
        first_far = jnp.where(first // 2 != hi, 1, 0)
        far_pair = 1 - first_far
        far_plane = jnp.where(first_far == 1, first, other)
        near_plane = jnp.where(first_far == 1, other, first)
        return far_pair, far_plane, near_plane

    def pair_copy(g):
        return pltpu.make_async_remote_copy(
            pair_out.at[g], pair_in.at[g], pair_s.at[g], pair_r.at[g],
            device_id=partner, device_id_type=MESH,
        )

    def mate_copy(q):
        return pltpu.make_async_remote_copy(
            mate_out.at[q], mate_in.at[q], mate_s.at[q], mate_r.at[q],
            device_id=partner, device_id_type=MESH,
        )

    def far_copy(g):
        _, far_plane, _ = planes(g)
        return pltpu.make_async_remote_copy(
            far_out.at[g], far_in.at[core, g // 2], far_s.at[g], far_r.at[core, g // 2],
            device_id=device(z, x, lo, hi + 1, far_plane), device_id_type=MESH,
        )

    def finish_pair(g):
        pair_copy(g).wait_recv()
        total = keep[g % 2] + pair_in[g].astype(jnp.float32)
        far_out[g] = total.astype(jnp.bfloat16)
        far_copy(g).start()

    blank = jnp.zeros((CAP, DK), jnp.bfloat16)
    ones = (
        (lax.broadcasted_iota(jnp.int32, (128, 256), 0) < CAP)
        == (lax.broadcasted_iota(jnp.int32, (128, 256), 1) < DK)
    ).astype(jnp.bfloat16)

    def group(g, _):
        base = g * 4
        for i in range(4):
            wait_partner(base + i)
        left = arr[0, pl.ds(base, 4)].reshape(256, HALF).astype(jnp.float32)
        right = arr[1, pl.ds(base, 4)].reshape(256, HALF).astype(jnp.float32)
        mean = (
            jnp.sum(left * left, axis=-1, keepdims=True)
            + jnp.sum(right * right, axis=-1, keepdims=True)
        ) / D
        scale = lax.rsqrt(mean + EPS)
        normed[:, 0:HALF] = (left * scale * gain_ref[:, 0:HALF]).astype(jnp.bfloat16)
        normed[:, HALF:D] = (right * scale * gain_ref[:, HALF:D]).astype(jnp.bfloat16)

        @pl.when(g == 0)
        def _():
            for copy in weights:
                copy.wait()

        rows = normed[...]
        query[...] = jnp.dot(rows, wq[...], preferred_element_type=jnp.float32).astype(jnp.bfloat16)
        key[...] = jnp.dot(rows, wk[...], preferred_element_type=jnp.float32).astype(jnp.bfloat16)
        value[...] = jnp.dot(rows, wv[...], preferred_element_type=jnp.float32).astype(jnp.bfloat16)

        @pl.when(g > 0)
        def _():
            finish_pair(g - 1)

        @pl.when(g < GROUPS - 1)
        def _():
            for i in range(4):
                receive(base + 4 + i)

        for block in range(2):
            code = jnp.where(west[0:1], codes[base + 2 * block], codes[base + 2 * block + 1])
            allowed = (row >= code // 256) & (row < code % 256)
            top = slice(block * 128, block * 128 + CAP)
            low = slice(block * 128 + CAP, block * 128 + 128)
            for h in range(HEADS):
                lanes = slice(h * DK, h * DK + DK)
                both = jnp.concatenate([query[top, lanes], query[low, lanes]], axis=1)
                keys = jnp.concatenate(
                    [
                        jnp.concatenate([key[top, lanes], blank], axis=1),
                        jnp.concatenate([blank, key[low, lanes]], axis=1),
                    ],
                    axis=0,
                )
                s = lax.dot_general(
                    both, keys, (((1,), (1,)), ((), ())), preferred_element_type=jnp.float32
                )
                scores[block, h] = jnp.where(allowed, s + bias[h], NEG)
        for block in range(2):
            for h in range(HEADS):
                s = scores[block, h]
                first = jnp.max(jnp.where(west, s, NEG), axis=-1, keepdims=True)
                second = jnp.max(jnp.where(west, NEG, s), axis=-1, keepdims=True)
                peak = jnp.maximum(jnp.where(west, first, second), 0.5 * NEG)
                probs[block, h] = jnp.exp(s - peak).astype(jnp.bfloat16)
        for block in range(2):
            top = slice(block * 128, block * 128 + CAP)
            low = slice(block * 128 + CAP, block * 128 + 128)
            sums = jnp.dot(
                probs[block].reshape(HEADS * CAP, 128), ones, preferred_element_type=jnp.float32
            )
            totals[block] = (1.0 / jnp.maximum(sums, 0.5)).reshape(HEADS, CAP, 256)
            for h in range(HEADS):
                lanes = slice(h * DK, h * DK + DK)
                values = jnp.concatenate(
                    [
                        jnp.concatenate([value[top, lanes], blank], axis=1),
                        jnp.concatenate([blank, value[low, lanes]], axis=1),
                    ],
                    axis=0,
                )
                ctx = jnp.dot(probs[block, h], values, preferred_element_type=jnp.float32)
                ctx = (ctx * totals[block, h]).astype(jnp.bfloat16)
                context[top, lanes] = ctx[:, 0:DK]
                context[low, lanes] = ctx[:, DK : 2 * DK]

        part[...] = jnp.dot(context[...], wo[...], preferred_element_type=jnp.float32)
        far_pair, _, near_plane = planes(g)
        far_rows = pl.ds(pl.multiple_of(far_pair * 128, 128), 128)
        near_rows = pl.ds(pl.multiple_of((1 - far_pair) * 128, 128), 128)
        own_cols = pl.ds(pl.multiple_of(core * HALF, HALF), HALF)
        other_cols = pl.ds(pl.multiple_of((1 - core) * HALF, HALF), HALF)
        pair_out[g] = part[far_rows, other_cols].astype(jnp.bfloat16)
        pair_copy(g).start()
        keep[g % 2] = part[far_rows, own_cols]

        @pl.when(near_plane % 2 == core)
        def _():
            mine[g // 2] = part[near_rows, :]

        @pl.when(near_plane % 2 != core)
        def _():
            mate_out[g // 2] = part[near_rows, :].astype(jnp.bfloat16)
            mate_copy(g // 2).start()

        return 0

    lax.fori_loop(0, GROUPS, group, 0)
    finish_pair(GROUPS - 1)

    plane = hi * 2 + core
    parity = (z + plane) % 2

    def combine(q, _):
        g = 2 * q + parity
        far_pair, _, _ = planes(g)
        near_pair = 1 - far_pair
        mate_copy(q).wait_recv()
        for c in range(2):
            pltpu.make_async_remote_copy(
                far_in.at[c, q], far_in.at[c, q], far_s.at[q], far_r.at[c, q],
                device_id=partner, device_id_type=MESH,
            ).wait_recv()
        for b in range(2):
            pos = g * 4 + near_pair * 2 + b
            _, dx, dl, _ = shift_of(pos)
            src_slot = ((x + 4 - dx) % 4) * 2 + (lo + dl) % 2
            span = slice(b * CAP, b * CAP + CAP)
            for c in range(2):
                cols = slice(c * HALF, c * HALF + HALF)
                total = (
                    mine[q, span, cols]
                    + mate_in[q, span, cols].astype(jnp.float32)
                    + far_in[c, q, span, :].astype(jnp.float32)
                    + arr[c, pos].astype(jnp.float32)
                )
                out_ref[src_slot, :, cols] = total.astype(jnp.bfloat16)
        return 0

    lax.fori_loop(0, 4, combine, 0)

    def drain(pos, _):
        @pl.when(pos != SELF)
        def _():
            token_copy(pos).wait_send()
            meta_copy(pos).wait_send()
            forward_copy(pos).wait_send()

        return 0

    own_forward.wait_send()
    lax.fori_loop(0, SLOTS, drain, 0)

    def drain_groups(g, _):
        pair_copy(g).wait_send()
        far_copy(g).wait_send()
        return 0

    lax.fori_loop(0, GROUPS, drain_groups, 0)

    def drain_mates(q, _):
        mate_copy(q).wait_send()
        return 0

    lax.fori_loop(0, 4, drain_mates, 0)


def layer(tenant, length, table, gain, tokens, wq, wk, wv, wo):
    pairs = tokens.shape[0]
    smem = pl.BlockSpec(memory_space=pltpu.SMEM)
    vmem = pl.BlockSpec(memory_space=pltpu.VMEM)
    anywhere = pl.BlockSpec(memory_space=pl.ANY)
    bf, f32 = jnp.bfloat16, jnp.float32
    dma = pltpu.SemaphoreType.DMA
    return pl.pallas_call(
        layer_kernel,
        out_shape=jax.ShapeDtypeStruct((8, CAP, D), bf),
        in_specs=[smem] * 3 + [vmem] + [anywhere] * 5,
        out_specs=vmem,
        scratch_shapes=[pltpu.VMEM((D, D), bf)] * 4
        + [
            pltpu.VMEM((pairs, CAP, HALF), bf),
            pltpu.VMEM((256, pairs * CAP), bf),
            pltpu.VMEM((SLOTS, CAP, HALF), bf),
            pltpu.VMEM((pairs * CAP // 128, 128), jnp.int32),
            pltpu.VMEM((SLOTS, 1, 128), jnp.int32),
            pltpu.VMEM((HEADS, CAP, 128), f32),
            pltpu.VMEM((2, SLOTS, CAP, HALF), bf),
            pltpu.VMEM((SLOTS, 1, 128), jnp.int32),
        ]
        + [pltpu.VMEM((256, D), bf)] * 5
        + [
            pltpu.VMEM((256, D), f32),
            pltpu.VMEM((2, HEADS, CAP, 128), f32),
            pltpu.VMEM((2, HEADS, CAP, 128), bf),
            pltpu.VMEM((2, HEADS, CAP, 256), f32),
            pltpu.VMEM((2, 128, HALF), f32),
            pltpu.VMEM((GROUPS, 128, HALF), bf),
            pltpu.VMEM((GROUPS, 128, HALF), bf),
            pltpu.VMEM((4, 128, D), bf),
            pltpu.VMEM((4, 128, D), bf),
            pltpu.VMEM((GROUPS, 128, HALF), bf),
            pltpu.VMEM((2, 4, 128, HALF), bf),
            pltpu.VMEM((4, 128, D), f32),
            dma((1,)), dma((4,)), dma((SLOTS,)), dma((SLOTS,)), dma((SLOTS,)), dma((SLOTS,)),
            dma((SLOTS,)), dma((SLOTS,)),
            dma((GROUPS,)), dma((GROUPS,)), dma((4,)), dma((4,)), dma((GROUPS,)), dma((2, 4)),
        ],
        compiler_params=pltpu.CompilerParams(
            collective_id=0, has_side_effects=True, vmem_limit_bytes=67_043_328
        ),
        name="layer",
    )(tenant, length, table, gain, tokens, wq, wk, wv, wo)


def per_device(
    src_tokens, pair_tenant, pair_length, norm_gain, w_query, w_key, w_value, w_out, rel_bias
):
    table = jnp.transpose(rel_bias[0])
    out = layer(
        pair_tenant, pair_length, table, norm_gain, src_tokens, w_query, w_key, w_value, w_out
    )
    return out.reshape(8 * CAP, D)


def solution(mesh):
    in_specs = (
        P("tenant", None, None),
        P("tenant"),
        P("tenant"),
        P("tenant", None),
        P("tenant", None, "tp"),
        P("tenant", None, "tp"),
        P("tenant", None, "tp"),
        P("tenant", "tp", None),
        P("tenant", None, "tp"),
    )
    out_specs = P(("tenant", "tp"), None)
    return jax.shard_map(
        per_device, mesh=mesh, in_specs=in_specs, out_specs=out_specs, check_vma=False
    )
```

```python
import functools
import math

import jax
import jax.numpy as jnp
import numpy as np
from jax import lax
from jax.experimental import pallas as pl
from jax.experimental.pallas import tpu as pltpu
from jax.sharding import PartitionSpec as P

MESH = pl.DeviceIdType.MESH
CAP = 64
D = 1024
HALF = 512
SLOTS = 32
GROUPS = 8
HEADS = 8
DK = 128
NEG = -1e30
EPS = 1e-6
BUCKETS = 32
SELF = 16


def bucket_limits():
    distance = np.arange(8, CAP)
    steps = np.floor(np.log(distance / 8) / math.log(16.0) * 8).astype(np.int32)
    steps = np.minimum(steps, 7)
    return [int(distance[steps >= n][0]) for n in range(1, int(steps.max()) + 1)]


def unrolled(count, body, carry):
    def steps(block, carry):
        for i in range(12):
            carry = body(block * 12 + i, carry)
        return carry

    return lax.fori_loop(0, count // 12, steps, carry)


def mod(a, b):
    return a % b if isinstance(a, int) else lax.rem(a, jnp.int32(b))


def div(a, b):
    return a // b if isinstance(a, int) else lax.div(a, jnp.int32(b))


def here():
    t = lax.axis_index("tenant")
    p = lax.axis_index("tp")
    return div(t, 8), mod(div(t, 2), 4), mod(t, 2), div(p, 2), mod(p, 2)


def device(z, x, lo, hi, core):
    return (mod(z, 4) * 8 + mod(x, 4) * 2 + mod(lo, 2), mod(hi, 2) * 2 + mod(core, 2))


def shift_of(pos):
    g = div(pos, 4)
    a = mod(div(pos, 2), 2)
    b = mod(pos, 2)
    odd_z = mod(g, 2)
    odd_x = mod(div(g, 2), 2)
    dl = 1 - div(g, 4)
    same = 1 - mod(odd_z + odd_x, 2)
    flip = dl * mod((same + (1 - same) * (1 - odd_z)) * a + (same + (1 - same) * odd_z) * b, 2)
    return odd_z + 2 * a, odd_x + 2 * b, dl, flip


def layer_kernel(
    tenant_ref, length_ref, table_ref, gain_ref, src_hbm, wq_hbm, wk_hbm, wv_hbm, wo_hbm, out_ref,
    wq, wk, wv, wo, tokens, pick, packed, spots, meta, bias,
    arr, codes, normed, query, key, value, context, part,
    scores, probs, totals, keep, pair_out, pair_in, mate_out, mate_in, far_out, far_in, mine,
    ssem, wsem, tok_s, tok_r, meta_s, meta_r, fwd_s, fwd_r,
    pair_s, pair_r, mate_s, mate_r, far_s, far_r,
):
    z, x, lo, hi, core = here()
    tenant = lax.axis_index("tenant")
    partner = device(z, x, lo, hi, core + 1)
    pairs = src_hbm.shape[0]
    chunks = pairs * CAP // 128

    def peer(pos):
        dz, dx, dl, flip = shift_of(pos)
        return device(z + dz, x + dx, lo + dl, hi + flip, core)

    source = pltpu.make_async_copy(
        src_hbm.at[:, :, pl.ds(pl.multiple_of(core * HALF, HALF), HALF)], tokens, ssem.at[0]
    )
    source.start()
    weights = [
        pltpu.make_async_copy(src.at[0], dst, wsem.at[i])
        for i, (src, dst) in enumerate(((wq_hbm, wq), (wk_hbm, wk), (wv_hbm, wv), (wo_hbm, wo)))
    ]
    for copy in weights:
        copy.start()

    barrier = pltpu.get_barrier_semaphore()

    for pos in range(SLOTS):
        if pos != SELF:
            pl.semaphore_signal(barrier, inc=1, device_id=peer(pos), device_id_type=MESH)
    pl.semaphore_signal(barrier, inc=1, device_id=partner, device_id_type=MESH)
    for c in range(2):
        pl.semaphore_signal(
            barrier, inc=1, device_id=device(z, x, lo, hi + 1, c), device_id_type=MESH
        )

    lane = lax.broadcasted_iota(jnp.int32, (chunks, 128), 1)
    pair_of = lax.broadcasted_iota(jnp.int32, (chunks, 128), 0) * 2 + lane // CAP
    place = lane % CAP
    slot_of = lax.broadcasted_iota(jnp.int32, (SLOTS, 128), 0)
    slot_row = lax.broadcasted_iota(jnp.int32, (SLOTS, 128), 1) % CAP

    def spread(j, carry):
        whose, count = carry
        here_now = pair_of == j
        return jnp.where(here_now, tenant_ref[j], whose), jnp.where(here_now, length_ref[j], count)

    nothing = jnp.zeros((chunks, 128), jnp.int32)
    whose, count = unrolled(pairs, spread, (nothing, nothing))

    def stack(j, carry):
        offset, fill, code = carry
        who, size = tenant_ref[j], length_ref[j]
        offset = offset + jnp.where((whose == who) & (pair_of > j), size, 0)
        hit = slot_of == who
        inside = hit & (slot_row >= fill) & (slot_row < fill + size)
        code = jnp.where(inside, fill * 257 + size, code)
        return offset, jnp.where(hit, fill + size, fill), code

    empty = jnp.zeros((SLOTS, 128), jnp.int32)
    offset, _, code = unrolled(pairs, stack, (nothing, empty, empty))
    spots[...] = jnp.where(place < count, whose * CAP + offset + place, -1)
    for u in range(SLOTS):
        meta[u] = code[u : u + 1, :]

    row = lax.broadcasted_iota(jnp.int32, (CAP, 128), 0)
    west = lax.broadcasted_iota(jnp.int32, (CAP, 128), 1) < CAP

    def pack(g):
        slots = [peer(g * 4 + s)[0] * CAP for s in range(4)]
        for m in range(chunks):
            spot = spots[m : m + 1, :]
            for s in range(4):
                pick[s * CAP : s * CAP + CAP, m * 128 : m * 128 + 128] = jnp.where(
                    row == spot - slots[s], 1.0, 0.0
                ).astype(jnp.bfloat16)
        rows = jnp.dot(
            pick[...], tokens[...].reshape(pairs * CAP, HALF), preferred_element_type=jnp.float32
        )
        packed[pl.ds(g * 4, 4)] = rows.astype(jnp.bfloat16).reshape(4, CAP, HALF)

    def token_copy(pos):
        target = peer(pos)
        return pltpu.make_async_remote_copy(
            packed.at[pos], arr.at[core, pos], tok_s.at[pos], tok_r.at[pos],
            device_id=target, device_id_type=MESH,
        )

    def meta_copy(pos):
        target = peer(pos)
        return pltpu.make_async_remote_copy(
            meta.at[target[0]], codes.at[pos], meta_s.at[pos], meta_r.at[pos],
            device_id=target, device_id_type=MESH,
        )

    def forward_copy(pos):
        return pltpu.make_async_remote_copy(
            arr.at[core, pos], arr.at[core, pos], fwd_s.at[pos], fwd_r.at[pos],
            device_id=partner, device_id_type=MESH,
        )

    own_forward = pltpu.make_async_remote_copy(
        packed.at[SELF], arr.at[core, SELF], fwd_s.at[SELF], fwd_r.at[SELF],
        device_id=partner, device_id_type=MESH,
    )

    def wait_partner(pos):
        pltpu.make_async_remote_copy(
            arr.at[1 - core, pos], arr.at[1 - core, pos], fwd_s.at[pos], fwd_r.at[pos],
            device_id=partner, device_id_type=MESH,
        ).wait_recv()

    def send(pos):
        @pl.when(pos != SELF)
        def _():
            meta_copy(pos).start()
            token_copy(pos).start()

    def send_group(g):
        for i in range(4):
            send(g * 4 + i)

    source.wait()
    pack(0)
    pl.semaphore_wait(barrier, SLOTS + 2)

    def pack_and_send(g, _):
        send_group(g - 1)
        pack(g)
        return 0

    lax.fori_loop(1, GROUPS, pack_and_send, 0)
    send_group(GROUPS - 1)
    own_forward.start()
    arr[core, SELF] = packed[SELF]
    codes[SELF] = meta[tenant]

    def receive(pos):
        @pl.when(pos != SELF)
        def _():
            token_copy(pos).wait_recv()
            meta_copy(pos).wait_recv()
            forward_copy(pos).start()

    for pos in range(4):
        receive(pos)

    ahead = lax.broadcasted_iota(jnp.int32, (CAP, 128), 1) % CAP - row
    distance = jnp.abs(ahead)
    bucket = jnp.where(distance < 8, distance, 8)
    for limit in bucket_limits():
        bucket = bucket + jnp.where(distance >= limit, 1, 0)
    bucket = bucket + jnp.where(ahead > 0, 16, 0)

    def expand(h, _):
        total = jnp.zeros((CAP, 128), jnp.float32)
        for k in range(BUCKETS):
            total = jnp.where(bucket == k, table_ref[h, k], total)
        bias[h] = total
        return 0

    lax.fori_loop(0, HEADS, expand, 0)

    def planes(g):
        first = (z + 4 - g % 2) % 4
        other = (first + 2) % 4
        first_far = jnp.where(first // 2 != hi, 1, 0)
        far_pair = 1 - first_far
        far_plane = jnp.where(first_far == 1, first, other)
        near_plane = jnp.where(first_far == 1, other, first)
        return far_pair, far_plane, near_plane

    def pair_copy(g):
        return pltpu.make_async_remote_copy(
            pair_out.at[g], pair_in.at[g], pair_s.at[g], pair_r.at[g],
            device_id=partner, device_id_type=MESH,
        )

    def mate_copy(q):
        return pltpu.make_async_remote_copy(
            mate_out.at[q], mate_in.at[q], mate_s.at[q], mate_r.at[q],
            device_id=partner, device_id_type=MESH,
        )

    def far_copy(g):
        _, far_plane, _ = planes(g)
        return pltpu.make_async_remote_copy(
            far_out.at[g], far_in.at[core, g // 2], far_s.at[g], far_r.at[core, g // 2],
            device_id=device(z, x, lo, hi + 1, far_plane), device_id_type=MESH,
        )

    def finish_pair(g):
        pair_copy(g).wait_recv()
        total = keep[g % 2] + pair_in[g].astype(jnp.float32)
        far_out[g] = total.astype(jnp.bfloat16)
        far_copy(g).start()

    blank = jnp.zeros((CAP, DK), jnp.bfloat16)
    ones = (
        (lax.broadcasted_iota(jnp.int32, (128, 256), 0) < CAP)
        == (lax.broadcasted_iota(jnp.int32, (128, 256), 1) < DK)
    ).astype(jnp.bfloat16)

    def group(g, _):
        base = g * 4
        for i in range(4):
            wait_partner(base + i)
        left = arr[0, pl.ds(base, 4)].reshape(256, HALF).astype(jnp.float32)
        right = arr[1, pl.ds(base, 4)].reshape(256, HALF).astype(jnp.float32)
        mean = (
            jnp.sum(left * left, axis=-1, keepdims=True)
            + jnp.sum(right * right, axis=-1, keepdims=True)
        ) / D
        scale = lax.rsqrt(mean + EPS)
        normed[:, 0:HALF] = (left * scale * gain_ref[:, 0:HALF]).astype(jnp.bfloat16)
        normed[:, HALF:D] = (right * scale * gain_ref[:, HALF:D]).astype(jnp.bfloat16)

        @pl.when(g == 0)
        def _():
            for copy in weights:
                copy.wait()

        rows = normed[...]
        query[...] = jnp.dot(rows, wq[...], preferred_element_type=jnp.float32).astype(jnp.bfloat16)
        key[...] = jnp.dot(rows, wk[...], preferred_element_type=jnp.float32).astype(jnp.bfloat16)
        value[...] = jnp.dot(rows, wv[...], preferred_element_type=jnp.float32).astype(jnp.bfloat16)

        @pl.when(g > 0)
        def _():
            finish_pair(g - 1)

        @pl.when(g < GROUPS - 1)
        def _():
            for i in range(4):
                receive(base + 4 + i)

        for block in range(2):
            code = jnp.where(west[0:1], codes[base + 2 * block], codes[base + 2 * block + 1])
            allowed = (row >= code // 256) & (row < code % 256)
            top = slice(block * 128, block * 128 + CAP)
            low = slice(block * 128 + CAP, block * 128 + 128)
            for h in range(HEADS):
                lanes = slice(h * DK, h * DK + DK)
                both = jnp.concatenate([query[top, lanes], query[low, lanes]], axis=1)
                keys = jnp.concatenate(
                    [
                        jnp.concatenate([key[top, lanes], blank], axis=1),
                        jnp.concatenate([blank, key[low, lanes]], axis=1),
                    ],
                    axis=0,
                )
                s = lax.dot_general(
                    both, keys, (((1,), (1,)), ((), ())), preferred_element_type=jnp.float32
                )
                scores[block, h] = jnp.where(allowed, s + bias[h], NEG)
        for block in range(2):
            for h in range(HEADS):
                s = scores[block, h]
                first = jnp.max(jnp.where(west, s, NEG), axis=-1, keepdims=True)
                second = jnp.max(jnp.where(west, NEG, s), axis=-1, keepdims=True)
                peak = jnp.maximum(jnp.where(west, first, second), 0.5 * NEG)
                probs[block, h] = jnp.exp(s - peak).astype(jnp.bfloat16)
        for block in range(2):
            top = slice(block * 128, block * 128 + CAP)
            low = slice(block * 128 + CAP, block * 128 + 128)
            sums = jnp.dot(
                probs[block].reshape(HEADS * CAP, 128), ones, preferred_element_type=jnp.float32
            )
            totals[block] = (1.0 / jnp.maximum(sums, 0.5)).reshape(HEADS, CAP, 256)
            for h in range(HEADS):
                lanes = slice(h * DK, h * DK + DK)
                values = jnp.concatenate(
                    [
                        jnp.concatenate([value[top, lanes], blank], axis=1),
                        jnp.concatenate([blank, value[low, lanes]], axis=1),
                    ],
                    axis=0,
                )
                ctx = jnp.dot(probs[block, h], values, preferred_element_type=jnp.float32)
                ctx = (ctx * totals[block, h]).astype(jnp.bfloat16)
                context[top, lanes] = ctx[:, 0:DK]
                context[low, lanes] = ctx[:, DK : 2 * DK]

        part[...] = jnp.dot(context[...], wo[...], preferred_element_type=jnp.float32)
        far_pair, _, near_plane = planes(g)
        far_rows = pl.ds(pl.multiple_of(far_pair * 128, 128), 128)
        near_rows = pl.ds(pl.multiple_of((1 - far_pair) * 128, 128), 128)
        own_cols = pl.ds(pl.multiple_of(core * HALF, HALF), HALF)
        other_cols = pl.ds(pl.multiple_of((1 - core) * HALF, HALF), HALF)
        pair_out[g] = part[far_rows, other_cols].astype(jnp.bfloat16)
        pair_copy(g).start()
        keep[g % 2] = part[far_rows, own_cols]

        @pl.when(near_plane % 2 == core)
        def _():
            mine[g // 2] = part[near_rows, :]

        @pl.when(near_plane % 2 != core)
        def _():
            mate_out[g // 2] = part[near_rows, :].astype(jnp.bfloat16)
            mate_copy(g // 2).start()

        return 0

    lax.fori_loop(0, GROUPS, group, 0)
    finish_pair(GROUPS - 1)

    plane = hi * 2 + core
    parity = (z + plane) % 2

    def combine(q, _):
        g = 2 * q + parity
        far_pair, _, _ = planes(g)
        near_pair = 1 - far_pair
        mate_copy(q).wait_recv()
        for c in range(2):
            pltpu.make_async_remote_copy(
                far_in.at[c, q], far_in.at[c, q], far_s.at[q], far_r.at[c, q],
                device_id=partner, device_id_type=MESH,
            ).wait_recv()
        for b in range(2):
            pos = g * 4 + near_pair * 2 + b
            _, dx, dl, _ = shift_of(pos)
            src_slot = ((x + 4 - dx) % 4) * 2 + (lo + dl) % 2
            span = slice(b * CAP, b * CAP + CAP)
            for c in range(2):
                cols = slice(c * HALF, c * HALF + HALF)
                total = (
                    mine[q, span, cols]
                    + mate_in[q, span, cols].astype(jnp.float32)
                    + far_in[c, q, span, :].astype(jnp.float32)
                    + arr[c, pos].astype(jnp.float32)
                )
                out_ref[src_slot, :, cols] = total.astype(jnp.bfloat16)
        return 0

    lax.fori_loop(0, 4, combine, 0)

    def drain(pos, _):
        @pl.when(pos != SELF)
        def _():
            token_copy(pos).wait_send()
            meta_copy(pos).wait_send()
            forward_copy(pos).wait_send()

        return 0

    own_forward.wait_send()
    lax.fori_loop(0, SLOTS, drain, 0)

    def drain_groups(g, _):
        pair_copy(g).wait_send()
        far_copy(g).wait_send()
        return 0

    lax.fori_loop(0, GROUPS, drain_groups, 0)

    def drain_mates(q, _):
        mate_copy(q).wait_send()
        return 0

    lax.fori_loop(0, 4, drain_mates, 0)


def layer(tenant, length, table, gain, tokens, wq, wk, wv, wo):
    pairs = tokens.shape[0]
    smem = pl.BlockSpec(memory_space=pltpu.SMEM)
    vmem = pl.BlockSpec(memory_space=pltpu.VMEM)
    anywhere = pl.BlockSpec(memory_space=pl.ANY)
    bf, f32 = jnp.bfloat16, jnp.float32
    dma = pltpu.SemaphoreType.DMA
    return pl.pallas_call(
        layer_kernel,
        out_shape=jax.ShapeDtypeStruct((8, CAP, D), bf),
        in_specs=[smem] * 3 + [vmem] + [anywhere] * 5,
        out_specs=vmem,
        scratch_shapes=[pltpu.VMEM((D, D), bf)] * 4
        + [
            pltpu.VMEM((pairs, CAP, HALF), bf),
            pltpu.VMEM((256, pairs * CAP), bf),
            pltpu.VMEM((SLOTS, CAP, HALF), bf),
            pltpu.VMEM((pairs * CAP // 128, 128), jnp.int32),
            pltpu.VMEM((SLOTS, 1, 128), jnp.int32),
            pltpu.VMEM((HEADS, CAP, 128), f32),
            pltpu.VMEM((2, SLOTS, CAP, HALF), bf),
            pltpu.VMEM((SLOTS, 1, 128), jnp.int32),
        ]
        + [pltpu.VMEM((256, D), bf)] * 5
        + [
            pltpu.VMEM((256, D), f32),
            pltpu.VMEM((2, HEADS, CAP, 128), f32),
            pltpu.VMEM((2, HEADS, CAP, 128), bf),
            pltpu.VMEM((2, HEADS, CAP, 256), f32),
            pltpu.VMEM((2, 128, HALF), f32),
            pltpu.VMEM((GROUPS, 128, HALF), bf),
            pltpu.VMEM((GROUPS, 128, HALF), bf),
            pltpu.VMEM((4, 128, D), bf),
            pltpu.VMEM((4, 128, D), bf),
            pltpu.VMEM((GROUPS, 128, HALF), bf),
            pltpu.VMEM((2, 4, 128, HALF), bf),
            pltpu.VMEM((4, 128, D), f32),
            dma((1,)), dma((4,)), dma((SLOTS,)), dma((SLOTS,)), dma((SLOTS,)), dma((SLOTS,)),
            dma((SLOTS,)), dma((SLOTS,)),
            dma((GROUPS,)), dma((GROUPS,)), dma((4,)), dma((4,)), dma((GROUPS,)), dma((2, 4)),
        ],
        compiler_params=pltpu.CompilerParams(
            collective_id=0, has_side_effects=True, vmem_limit_bytes=67_043_328
        ),
        name="layer",
    )(tenant, length, table, gain, tokens, wq, wk, wv, wo)


def per_device(
    src_tokens, pair_tenant, pair_length, norm_gain, w_query, w_key, w_value, w_out, rel_bias
):
    table = jnp.transpose(rel_bias[0])
    out = layer(
        pair_tenant, pair_length, table, norm_gain, src_tokens, w_query, w_key, w_value, w_out
    )
    return out.reshape(8 * CAP, D)


def solution(mesh):
    in_specs = (
        P("tenant", None, None),
        P("tenant"),
        P("tenant"),
        P("tenant", None),
        P("tenant", None, "tp"),
        P("tenant", None, "tp"),
        P("tenant", None, "tp"),
        P("tenant", "tp", None),
        P("tenant", None, "tp"),
    )
    out_specs = P(("tenant", "tp"), None)
    return jax.shard_map(
        per_device, mesh=mesh, in_specs=in_specs, out_specs=out_specs, check_vma=False
    )
```
